32 devices in a mesh: items: 2 (over x), rows: 16 (over z, y, core).
Axes of the slice: x: 2, y: 2, z: 4, core: 2. Of those that a mesh axis runs over, the one named last changes fastest.
Arguments:
- patches: bfloat16 [128, 32, 1152], P(('items', 'rows')), may hold values from -6 to 6
- condition: bfloat16 [4, 1152], P('items'), may hold values from -6 to 6
- lengths: int32 [4], P('items'), may hold values from 256 to 1024, as said below
- modulator: bfloat16 [1152, 6912], P(None, 'rows'), may hold values from -0.1875 to 0.1875
- baseline: float32 [6912], P('rows'), may hold values from -4 to 4
- projector: bfloat16 [1152, 3456], P('rows'), may hold values from -0.1875 to 0.1875
- forgetter: bfloat16 [1152, 16], P('rows'), may hold values from -0.1875 to 0.1875
- retention: float32 [16], replicated, may hold values from 0.5 to 5
- smoother: float32 [9, 1152], replicated, may hold values from -6 to 6
- pedestal: float32 [1152], replicated, may hold values from -16 to 16
- combiner: bfloat16 [1152, 1152], P('rows'), may hold values from -0.005859375 to 0.005859375
- displacement: float32 [1152], replicated, may hold values from -4 to 4
- expander: bfloat16 [1152, 4608], P('rows'), may hold values from -0.1875 to 0.1875
- thresholds: float32 [4608], replicated, may hold values from -4 to 4
- reducer: bfloat16 [4608, 1152], P('rows'), may hold values from -0.09375 to 0.09375
- leveling: float32 [1152], replicated, may hold values from -4 to 4
- cotangent: bfloat16 [128, 32, 1152], P(('items', 'rows')), may hold values from -6 to 6
Outputs:
- block_output: bfloat16 [128, 32, 1152], P(('items', 'rows'))
- patches_grad: bfloat16 [128, 32, 1152], P(('items', 'rows'))
- condition_grad: float32 [4, 1152], P('items')
- modulator_grad: float32 [1152, 6912], P(None, 'rows')
- baseline_grad: float32 [6912], P('rows')
- projector_grad: float32 [1152, 3456], P('rows')
- forgetter_grad: float32 [1152, 16], P('rows')
- retention_grad: float32 [16], replicated
- smoother_grad: float32 [9, 1152], replicated
- pedestal_grad: float32 [1152], replicated
- combiner_grad: float32 [1152, 1152], P('rows')
- displacement_grad: float32 [1152], replicated
- expander_grad: float32 [1152, 4608], P('rows')
- thresholds_grad: float32 [4608], replicated
- reducer_grad: float32 [4608, 1152], P('rows')
- leveling_grad: float32 [1152], replicated
The draws below stay inside these ranges and needn't reach their ends.
Inputs may be any that keep to these rules, and one draw needn't show every extreme that they name: lengths[b] counts the valid patches of item b, the first ones in row-major place; in every draw some item has all 1024 valid.
All inputs are finite; a program needn't handle non-finite values.
Results may differ from the reference program's by a relative error of at most 0.018.
Values may be sent and summed in bfloat16 or wider, within the bound.
A program may use at most 256 MiB of HBM per device.

```python
import math
import jax
import jax.numpy as jnp
from jax import lax

H = 16
HD = 72
D = 1152
FF = 4608
GRID = 32
PATCHES = 1024
TRACT = 64
ITEMS = 4
PROWS = 128


def draw_lengths(key, part):
    first_key, second_key = jax.random.split(key)
    drawn = jax.random.randint(first_key, (ITEMS,), PATCHES // 4, PATCHES + 1)
    chosen = jax.random.randint(second_key, (), 0, ITEMS)
    return jnp.where(jnp.arange(ITEMS) == chosen, PATCHES, drawn).astype(jnp.int32)


def levels(stream_key, shape, cuts, low, largest):
    gain = 1.0
    for axis_at, parts in cuts:
        draws = jax.random.uniform(jax.random.fold_in(jax.random.fold_in(stream_key, 6), axis_at), (parts,), jnp.float32, low / len(cuts), largest / len(cuts))
        gain = gain * jnp.repeat(jnp.exp(draws), shape[axis_at] // parts).reshape((-1,) + (1,) * (len(shape) - 1 - axis_at))
    return gain


def scatter_about(own_key, dims, scale, most, cuts=(), held_as=jnp.bfloat16):
    level = levels(own_key, dims, cuts, -0.22, 0.18) if cuts else 1.0
    values = jax.random.normal(own_key, dims, jnp.float32) * scale * level
    return jnp.minimum(jnp.maximum(values, -most), most).astype(held_as)


def setup_inputs(seed: int = 0) -> dict:
    seeds = jax.random.split(jax.random.key(seed), 18)
    patches = scatter_about(seeds[0], (PROWS, GRID, D), 1.0, 6.0, ((0, 32),))
    condition = scatter_about(seeds[1], (ITEMS, D), 1.0, 6.0, ((0, 2),))
    lengths = draw_lengths(jax.random.fold_in(seeds[17], 71), 0)
    modulator = scatter_about(seeds[3], (D, 6 * D), D ** -0.5, 0.1875, ((1, 16),))
    baseline = scatter_about(seeds[4], (6 * D,), 0.3, 4.0, ((0, 16),), jnp.float32)
    projector = scatter_about(seeds[5], (D, 3 * D), D ** -0.5, 0.1875, ((0, 16),))
    forgetter = scatter_about(seeds[6], (D, H), D ** -0.5, 0.1875, ((0, 16),))
    retention = jnp.clip(jax.random.uniform(seeds[7], (H,), jnp.float32, 0.5, 5.0), 0.5, 5.0)
    smoother = scatter_about(seeds[8], (9, D), 0.4, 6.0, (), jnp.float32)
    pedestal = scatter_about(seeds[9], (D,), 3.0, 16.0, (), jnp.float32)
    combiner = scatter_about(seeds[10], (D, D), (1024 * D) ** -0.5, 0.005859375, ((0, 16),))
    displacement = scatter_about(seeds[11], (D,), 0.3, 4.0, (), jnp.float32)
    expander = scatter_about(seeds[12], (D, FF), D ** -0.5, 0.1875, ((0, 16),))
    thresholds = scatter_about(seeds[13], (FF,), 0.3, 4.0, (), jnp.float32)
    reducer = scatter_about(seeds[14], (FF, D), FF ** -0.5, 0.09375, ((0, 16),))
    leveling = scatter_about(seeds[15], (D,), 0.3, 4.0, (), jnp.float32)
    cotangent = scatter_about(seeds[16], (PROWS, GRID, D), 1.0, 6.0, ((0, 32),))
    return {"patches": patches, "condition": condition, "lengths": lengths, "modulator": modulator, "baseline": baseline, "projector": projector, "forgetter": forgetter, "retention": retention, "smoother": smoother, "pedestal": pedestal, "combiner": combiner, "displacement": displacement, "expander": expander, "thresholds": thresholds, "reducer": reducer, "leveling": leveling, "cotangent": cotangent}


EPS = 1e-06
HIGH = lax.Precision.HIGHEST

@jax.custom_vjp
def low(v):
    return lax.optimization_barrier(v.astype(jnp.bfloat16)).astype(jnp.float32)

@jax.custom_vjp
def low_back(v):
    return v

def low_keep(v):
    return (low(v), None)

def low_pass(kept, grad):
    return (grad,)

def back_keep(v):
    return (v, None)

def back_low(kept, grad):
    return (low(grad),)
low.defvjp(low_keep, low_pass)
low_back.defvjp(back_keep, back_low)

def layer_norm(values):
    centred = values - lax.optimization_barrier(jnp.mean(values, axis=-1, keepdims=True))
    return centred * lax.rsqrt(lax.optimization_barrier(jnp.mean(centred * centred, axis=-1, keepdims=True)) + EPS)

def tract_step(carried, pieces):
    queries, key_rows, values, decays = pieces
    length = queries.shape[1]
    summed = jnp.cumsum(decays, axis=1)
    totals = summed[:, -1]
    factor = queries.shape[-1] ** (-0.5)
    scores = jnp.einsum('bik,bjk->bij', queries, key_rows, precision=HIGH)
    causal = jnp.arange(length)[:, None] >= jnp.arange(length)[None, :]
    offsets = jnp.where(causal, summed[:, :, None] - summed[:, None, :], 0.0)
    weights = jnp.where(causal, jnp.exp(offsets), 0.0)
    inside = jnp.einsum('bij,bjv->biv', scores * weights, values, precision=HIGH)
    carried_in = jnp.einsum('bik,bkv->biv', queries, carried, precision=HIGH) * jnp.exp(summed)[:, :, None]
    outputs = (inside + carried_in) * factor
    fading = jnp.exp(totals[:, None] - summed)[:, :, None]
    carried_next = jnp.exp(totals)[:, None, None] * carried + jnp.einsum('bjk,bjv->bkv', key_rows * fading, values, precision=HIGH)
    return (carried_next, outputs)

def linear_attention(queries, key_rows, values, decays):
    leading = queries.shape[0]
    tract_count = queries.shape[1] // TRACT

    def blocks(source):
        shaped = source.reshape((leading, tract_count, TRACT) + source.shape[2:])
        return jnp.moveaxis(shaped, 1, 0)
    initial = jnp.zeros((leading, queries.shape[2], values.shape[2]), jnp.float32)
    last_state, outputs = lax.scan(jax.checkpoint(tract_step), initial, (blocks(queries), blocks(key_rows), blocks(values), blocks(decays)))
    return jnp.moveaxis(outputs, 0, 1).reshape(values.shape)

def smooth_grid(grid, smoother, pedestal):
    row_count = grid.shape[1]
    column_count = grid.shape[2]
    padded = jnp.pad(grid, ((0, 0), (1, 1), (1, 1), (0, 0)))
    result = jnp.zeros_like(grid) + pedestal
    for tap_index in range(9):
        down_by = tap_index // 3
        right_by = tap_index % 3
        result = result + smoother[tap_index] * padded[:, down_by:down_by + row_count, right_by:right_by + column_count]
    return result

def forward(patches, condition, lengths, modulator, baseline, projector, forgetter, retention, smoother, pedestal, combiner, displacement, expander, thresholds, reducer, leveling):
    leading = patches.shape[0]
    squashed = low(jax.nn.silu(condition))
    modulation = low(jnp.dot(squashed, modulator, precision=HIGH) + baseline)
    shift_one, scale_one, gate_one, shift_two, scale_two, gate_two = [modulation[:, None, None, part_index * D:(part_index + 1) * D] for part_index in range(6)]
    hidden = low(layer_norm(patches) * (1.0 + scale_one) + shift_one)
    projected = jnp.einsum('brcd,de->brce', hidden, projector, precision=HIGH)
    queries = low_back(low(projected[..., :D]))
    key_rows = low_back(low(projected[..., D:2 * D]))
    values = low_back(low(projected[..., 2 * D:]))
    forget_logit = low_back(jnp.einsum('brcd,dh->brch', hidden, forgetter, precision=HIGH) + retention)
    decays = low(jax.nn.log_sigmoid(forget_logit) / 16.0)
    places = jnp.arange(GRID)[:, None] * GRID + jnp.arange(GRID)[None, :]
    validity = (places[None] < lengths[:, None, None]).astype(jnp.float32)[..., None]
    key_rows = key_rows * validity
    values = values * validity

    def columns(source):
        shaped = jnp.swapaxes(source, 1, 2).reshape(leading, PATCHES, H, HD)
        return jnp.moveaxis(shaped, 2, 1).reshape(leading * H, PATCHES, HD)
    decay_columns = jnp.moveaxis(jnp.swapaxes(decays, 1, 2).reshape(leading, PATCHES, H), 2, 1).reshape(leading * H, PATCHES)
    attended = linear_attention(columns(queries), columns(key_rows), columns(values), decay_columns)
    attended = jnp.moveaxis(attended.reshape(leading, H, GRID, GRID, HD), 1, 3)
    attended = jnp.swapaxes(attended, 1, 2).reshape(leading, GRID, GRID, D)
    attended = low_back(low(attended))
    smoothed = low_back(low(smooth_grid(attended, smoother, pedestal)))
    branch = low_back(jnp.einsum('brcd,de->brce', smoothed, combiner, precision=HIGH) + displacement)
    middle = patches + gate_one * branch
    hidden_two = low(layer_norm(middle) * (1.0 + scale_two) + shift_two)
    expanded = low_back(jnp.einsum('brcd,de->brce', hidden_two, expander, precision=HIGH) + thresholds)
    activated = low(jax.nn.gelu(expanded, approximate=True))
    reduced = low_back(jnp.einsum('brce,ed->brcd', activated, reducer, precision=HIGH) + leveling)
    return middle + gate_two * reduced

def reference(patches, condition, lengths, modulator, baseline, projector, forgetter, retention, smoother, pedestal, combiner, displacement, expander, thresholds, reducer, leveling, cotangent):
    patch_grid = patches.astype(jnp.float32).reshape(ITEMS, GRID, GRID, D)
    grad_grid = cotangent.astype(jnp.float32).reshape(ITEMS, GRID, GRID, D)
    condition_float = condition.astype(jnp.float32)
    params = tuple((weight.astype(jnp.float32) for weight in (modulator, baseline, projector, forgetter, retention, smoother, pedestal, combiner, displacement, expander, thresholds, reducer, leveling)))
    per_step = math.gcd(ITEMS, 4)

    def by_steps(source):
        return source.reshape((ITEMS // per_step, per_step) + source.shape[1:])

    def advance(totals, block):
        block_patches, block_condition, block_lengths, block_grad = block

        def wrapped(inputs_patches, inputs_condition, *weights):
            return forward(inputs_patches, inputs_condition, block_lengths, *weights)
        result, pullback = jax.vjp(wrapped, block_patches, block_condition, *params)
        grads = pullback(block_grad)
        totals = tuple((left + right for left, right in zip(totals, grads[2:])))
        return (totals, (result, grads[0], grads[1]))
    zeros_start = tuple((jnp.zeros_like(weight) for weight in params))
    totals, (results, patch_grads, condition_grads) = lax.scan(advance, zeros_start, (by_steps(patch_grid), by_steps(condition_float), by_steps(lengths), by_steps(grad_grid)))
    block_output = results.reshape(PROWS, GRID, D).astype(jnp.bfloat16)
    patches_grad = patch_grads.reshape(PROWS, GRID, D).astype(jnp.bfloat16)
    condition_grad = condition_grads.reshape(ITEMS, D)
    return (block_output, patches_grad, condition_grad, totals[0], totals[1], totals[2], totals[3], totals[4], totals[5], totals[6], totals[7], totals[8], totals[9], totals[10], totals[11], totals[12])
```

```python
import functools

import jax
import jax.numpy as jnp
from jax import lax
from jax.experimental import pallas as pl
from jax.experimental.pallas import tpu as pltpu
from jax.sharding import Mesh, PartitionSpec as P

H = 16
HD = 72
D = 1152
FF = 4608
GRID = 32
PATCHES = 1024
ROWS_DEV = 4
TOK_DEV = 128
TEAM = GRID // ROWS_DEV
HEADS = H // TEAM
LANES = 128
WIDE = HEADS * LANES
STRIP = 256

EPS = 1e-06
HIGH = lax.Precision.HIGHEST
F32 = jnp.float32
BF16 = jnp.bfloat16
FACTOR = HD ** (-0.5)


def modulate(values, offset, stretch):
    centred = values - jnp.mean(values, axis=-1, keepdims=True)
    spread = jnp.mean(centred * centred, axis=-1, keepdims=True)
    return centred * lax.rsqrt(spread + EPS) * (1.0 + stretch) + offset


def dot(left, right):
    return jnp.dot(left, right, preferred_element_type=F32)


def outer_sum(left, right):
    return lax.dot_general(left, right, (((0,), (0,)), ((), ())), preferred_element_type=F32)


def back_dot(gradient, matrix):
    return lax.dot_general(gradient, matrix, (((1,), (1,)), ((), ())), preferred_element_type=F32)


def column_place(index):
    return (index & (GRID - 1)) * GRID + (index >> 5)


def strip_weights(start, gcol, grow):
    rows = lax.broadcasted_iota(jnp.int32, (STRIP, PATCHES), 0) + start
    cols = lax.broadcasted_iota(jnp.int32, (STRIP, PATCHES), 1)
    causal = column_place(cols) <= column_place(rows)
    return jnp.exp(jnp.where(causal, gcol - grow, -1e30))


def attend_kernel(q_ref, k_ref, v_ref, gcol_ref, grow_ref, out_ref):
    keys = k_ref[...]
    values = v_ref[...]
    grow = grow_ref[0]

    def strip(number, carry):
        start = pl.multiple_of(number * STRIP, STRIP)
        here = pl.ds(start, STRIP)
        weights = strip_weights(start, gcol_ref[0, here, :], grow)
        scores = back_dot(q_ref[here, :], keys) * weights
        out_ref[here, :] = (dot(scores.astype(BF16), values) * FACTOR).astype(BF16)
        return carry

    lax.fori_loop(0, PATCHES // STRIP, strip, 0)


def attend_back_kernel(
    q_ref, k_ref, v_ref, gcol_ref, grow_ref, do_ref, dq_ref, dk_ref, dv_ref, row_ref, col_ref
):
    keys = k_ref[...]
    values = v_ref[...]
    grow = grow_ref[0]
    dk_ref[...] = jnp.zeros_like(dk_ref)
    dv_ref[...] = jnp.zeros_like(dv_ref)
    col_ref[...] = jnp.zeros_like(col_ref)

    def strip(number, carry):
        start = pl.multiple_of(number * STRIP, STRIP)
        here = pl.ds(start, STRIP)
        queries = q_ref[here, :]
        grads = do_ref[here, :]
        weights = strip_weights(start, gcol_ref[0, here, :], grow)
        scores = back_dot(queries, keys) * weights
        back = back_dot(grads, values)
        pulled = (back * weights).astype(BF16)
        moment = back * scores
        dv_ref[...] += outer_sum(scores.astype(BF16), grads)
        dk_ref[...] += outer_sum(pulled, queries)
        dq_ref[here, :] = dot(pulled, keys) * FACTOR
        row_ref[0, here, :] = jnp.sum(moment, axis=1, keepdims=True) * FACTOR
        col_ref[0] += jnp.sum(moment, axis=0, keepdims=True) * FACTOR
        return carry

    lax.fori_loop(0, PATCHES // STRIP, strip, 0)
    dk_ref[...] *= FACTOR
    dv_ref[...] *= FACTOR


def head_specs():
    return [
        pl.BlockSpec((PATCHES, LANES), lambda h: (0, h)),
        pl.BlockSpec((PATCHES, LANES), lambda h: (0, HEADS + h)),
        pl.BlockSpec((PATCHES, LANES), lambda h: (0, 2 * HEADS + h)),
        pl.BlockSpec((1, PATCHES, 1), lambda h: (h, 0, 0)),
        pl.BlockSpec((1, 1, PATCHES), lambda h: (h, 0, 0)),
    ]


def attend(qkv, gcol, grow):
    return pl.pallas_call(
        attend_kernel,
        grid=(HEADS,),
        out_shape=jax.ShapeDtypeStruct((PATCHES, WIDE), BF16),
        in_specs=head_specs(),
        out_specs=pl.BlockSpec((PATCHES, LANES), lambda h: (0, h)),
        cost_estimate=pl.CostEstimate(
            flops=HEADS * 4 * PATCHES * PATCHES * LANES,
            bytes_accessed=8 * PATCHES * WIDE,
            transcendentals=HEADS * PATCHES * PATCHES,
        ),
        name="attend",
    )(qkv, qkv, qkv, gcol, grow)


def attend_back(qkv, gcol, grow, grads):
    block = pl.BlockSpec((PATCHES, LANES), lambda h: (0, h))
    return pl.pallas_call(
        attend_back_kernel,
        grid=(HEADS,),
        out_shape=[jax.ShapeDtypeStruct((PATCHES, WIDE), F32)] * 3
        + [
            jax.ShapeDtypeStruct((HEADS, PATCHES, 1), F32),
            jax.ShapeDtypeStruct((HEADS, 1, PATCHES), F32),
        ],
        in_specs=head_specs() + [block],
        out_specs=[block, block, block]
        + [
            pl.BlockSpec((1, PATCHES, 1), lambda h: (h, 0, 0)),
            pl.BlockSpec((1, 1, PATCHES), lambda h: (h, 0, 0)),
        ],
        cost_estimate=pl.CostEstimate(
            flops=HEADS * 10 * PATCHES * PATCHES * LANES,
            bytes_accessed=20 * PATCHES * WIDE,
            transcendentals=HEADS * PATCHES * PATCHES,
        ),
        name="attend_back",
    )(qkv, qkv, qkv, gcol, grow, grads)


def pad_heads(source, axis):
    widths = [(0, 0)] * source.ndim
    widths[axis] = (0, LANES - HD)
    return jnp.pad(source, widths)


def pad_cells(grid):
    return jnp.pad(grid, ((1, 1), (1, 1), (0, 0)))


def pick(source, axis, index):
    return lax.dynamic_index_in_dim(source, index, axis, keepdims=False)


def gather_tokens(source):
    return lax.all_gather(source, "pos", axis=0, tiled=True)


def scatter_tokens(partial):
    pieces = partial.astype(BF16).reshape(TEAM, TOK_DEV, D)
    arrived = lax.all_to_all(pieces, "pos", split_axis=0, concat_axis=0, tiled=True)
    return jnp.sum(arrived.astype(F32), axis=0)


def on_device(
    groups,
    patches,
    condition,
    lengths,
    modulator,
    baseline,
    projector,
    forgetter,
    retention,
    smoother,
    pedestal,
    combiner,
    displacement,
    expander,
    thresholds,
    reducer,
    leveling,
    cotangent,
):
    rows_axes = ("grp", "pos")
    half = lax.axis_index("items")
    halves = lax.axis_size("items")
    group = lax.axis_index("grp")
    place = lax.axis_index("pos")
    devices = groups * TEAM
    depth = D // devices
    inner = FF // devices
    columns = 6 * D // devices
    whole_heads = depth == HD
    upstream = cotangent.astype(F32).reshape(TOK_DEV, D)
    inputs = patches.astype(F32).reshape(TOK_DEV, D)

    condition_float = condition.astype(F32)
    squashed = jax.nn.silu(condition_float).astype(BF16)
    modulation_piece = (dot(squashed, modulator) + baseline).astype(BF16).T
    modulation_all = lax.all_gather(modulation_piece, rows_axes, axis=0, tiled=True)
    modulation = pick(modulation_all, 1, group).astype(F32)
    shift_one, scale_one, gate_one, shift_two, scale_two, gate_two = [
        modulation[part * D : (part + 1) * D] for part in range(6)
    ]

    project_cut = jnp.concatenate(
        [
            projector.reshape(depth, 3, HEADS, TEAM, HD)
            .transpose(3, 0, 1, 2, 4)
            .reshape(TEAM, depth, 3 * HEADS * HD),
            forgetter.reshape(depth, HEADS, TEAM).transpose(2, 0, 1),
        ],
        axis=2,
    )
    project_part = lax.all_to_all(project_cut, "pos", split_axis=0, concat_axis=0, tiled=True)
    project_mine = lax.all_gather(project_part, "grp", axis=0, tiled=True).reshape(D, -1)
    project_wide = jnp.concatenate(
        [
            pad_heads(project_mine[:, : 3 * HEADS * HD].reshape(D, 3 * HEADS, HD), 2).reshape(
                D, 3 * WIDE
            ),
            jnp.pad(project_mine[:, 3 * HEADS * HD :], ((0, 0), (0, LANES - HEADS))),
        ],
        axis=1,
    )
    expand_cut = (
        expander.reshape(depth, groups, TEAM, inner)
        .transpose(2, 0, 1, 3)
        .reshape(TEAM, depth, groups * inner)
    )
    expand_part = lax.all_to_all(expand_cut, "pos", split_axis=0, concat_axis=0, tiled=True)
    expand_mine = lax.all_gather(expand_part, "grp", axis=0, tiled=True).reshape(D, groups * inner)
    reduce_mine = lax.all_gather(reducer, "grp", axis=0, tiled=True)
    if whole_heads:
        combine_mine = lax.all_gather(combiner, "grp", axis=0, tiled=True).reshape(HEADS, HD, D)
    else:
        combine_all = lax.all_gather(combiner, rows_axes, axis=0, tiled=True)
        combine_mine = pick(combine_all.reshape(HEADS, TEAM, HD, D), 1, place)
    combine_wide = pad_heads(combine_mine, 1).reshape(WIDE, D)
    thresholds_mine = pick(thresholds.reshape(groups, TEAM, inner), 1, place).reshape(-1)
    retention_mine = pick(retention.reshape(HEADS, TEAM), 1, place)
    kernel = pad_heads(pick(smoother.reshape(9, HEADS, TEAM, HD), 2, place), 2).reshape(9, WIDE)
    offset = pad_heads(pick(pedestal.reshape(HEADS, TEAM, HD), 1, place), 1).reshape(WIDE)

    hidden = modulate(inputs, shift_one, scale_one).astype(BF16)
    hidden_all = gather_tokens(hidden)
    projected = dot(hidden_all, project_wide)
    forget_logit = projected[:, 3 * WIDE : 3 * WIDE + HEADS] + retention_mine
    decays = (jax.nn.log_sigmoid(forget_logit) / 16.0).astype(BF16)
    index = jnp.arange(PATCHES, dtype=jnp.int32)
    length = pick(lengths, 0, group)
    validity = (index < length)[:, None]
    is_query = jnp.arange(3 * WIDE) < WIDE
    keep = validity | is_query[None, :]
    qkv = jnp.where(keep, projected[:, : 3 * WIDE], 0.0).astype(BF16)
    order = column_place(index)
    causal = (order[None, :] <= order[:, None]).astype(BF16)
    summed = dot(causal, decays)
    gcol = summed.T[:, :, None]
    grow = summed.T[:, None, :]
    attended = attend(qkv, gcol, grow)

    attended_grid = attended.astype(F32).reshape(GRID, GRID, WIDE)
    attended_padded = pad_cells(attended_grid)
    smoothed = jnp.zeros_like(attended_grid) + offset
    for tap in range(9):
        down, right = tap // 3, tap % 3
        smoothed = (
            smoothed + kernel[tap] * attended_padded[down : down + GRID, right : right + GRID]
        )
    smoothed = smoothed.astype(BF16).reshape(PATCHES, WIDE)
    branch = scatter_tokens(dot(smoothed, combine_wide)) + displacement
    middle = inputs + gate_one * branch
    hidden_two = modulate(middle, shift_two, scale_two).astype(BF16)
    hidden_two_all = gather_tokens(hidden_two)
    expanded = dot(hidden_two_all, expand_mine) + thresholds_mine
    activated = jax.nn.gelu(expanded, approximate=True).astype(BF16)
    reduced = scatter_tokens(dot(activated, reduce_mine)) + leveling
    block_output = (middle + gate_two * reduced).astype(BF16).reshape(ROWS_DEV, GRID, D)

    gate_two_grad = jnp.sum(upstream * reduced, axis=0)
    reduced_grad = (gate_two * upstream).astype(BF16)
    leveling_grad = jnp.sum(reduced_grad.astype(F32), axis=0)
    reduced_grad_all = gather_tokens(reduced_grad)
    reducer_grad = outer_sum(activated, reduced_grad_all)
    activated_grad = back_dot(reduced_grad_all, reduce_mine)
    pull = jax.vjp(lambda v: jax.nn.gelu(v, approximate=True), expanded)[1]
    expanded_grad = pull(activated_grad)[0].astype(BF16)
    thresholds_grad = jnp.sum(expanded_grad.astype(F32), axis=0)
    expander_grad = outer_sum(hidden_two_all, expanded_grad)
    hidden_two_grad = scatter_tokens(back_dot(expanded_grad, expand_mine))
    second_pull = jax.vjp(modulate, middle, shift_two, scale_two)[1]
    middle_part, shift_two_grad, scale_two_grad = second_pull(hidden_two_grad)
    middle_grad = upstream + middle_part
    gate_one_grad = jnp.sum(middle_grad * branch, axis=0)
    branch_grad = (gate_one * middle_grad).astype(BF16)
    displacement_grad = jnp.sum(branch_grad.astype(F32), axis=0)
    branch_grad_all = gather_tokens(branch_grad)
    combiner_grad = outer_sum(smoothed, branch_grad_all)
    smoothed_grad = back_dot(branch_grad_all, combine_wide).astype(BF16).astype(F32)
    pedestal_grad = jnp.sum(smoothed_grad, axis=0)
    grad_grid = smoothed_grad.reshape(GRID, GRID, WIDE)
    grad_padded = pad_cells(grad_grid)
    tap_grads = []
    attended_grad = jnp.zeros_like(grad_grid)
    for tap in range(9):
        down, right = tap // 3, tap % 3
        tap_grads.append(
            jnp.sum(
                grad_grid * attended_padded[down : down + GRID, right : right + GRID], axis=(0, 1)
            )
        )
        attended_grad = (
            attended_grad
            + kernel[tap] * grad_padded[2 - down : 2 - down + GRID, 2 - right : 2 - right + GRID]
        )
    tap_stack = jnp.stack(tap_grads)
    attended_grad = attended_grad.astype(BF16).reshape(PATCHES, WIDE)
    dq, dk, dv, row_sum, col_sum = attend_back(qkv, gcol, grow, attended_grad)
    moment = row_sum[:, :, 0] - col_sum[:, 0, :]
    decay_grad = lax.dot_general(
        causal.astype(F32),
        moment,
        (((0,), (1,)), ((), ())),
        precision=HIGH,
        preferred_element_type=F32,
    )
    forget_grad = (decay_grad * jax.nn.sigmoid(-forget_logit) / 16.0).astype(BF16)
    retention_grad = jnp.sum(forget_grad.astype(F32), axis=0)
    project_grad = jnp.concatenate(
        [
            dq.astype(BF16),
            jnp.where(validity, dk, 0.0).astype(BF16),
            jnp.where(validity, dv, 0.0).astype(BF16),
            jnp.pad(forget_grad, ((0, 0), (0, LANES - HEADS))),
        ],
        axis=1,
    )
    projector_grad = outer_sum(hidden_all, project_grad)
    hidden_grad = scatter_tokens(back_dot(project_grad, project_wide))
    first_pull = jax.vjp(modulate, inputs, shift_one, scale_one)[1]
    inputs_part, shift_one_grad, scale_one_grad = first_pull(hidden_grad)
    patches_grad = (middle_grad + inputs_part).astype(BF16).reshape(ROWS_DEV, GRID, D)

    def swap_add(share):
        low = share.astype(BF16)
        other = lax.ppermute(low, "items", [(i, (i + 1) % 2) for i in range(2)])
        return low.astype(F32) + other.astype(F32)

    def to_owners(source):
        pieces = source.reshape(devices, depth, source.shape[1])
        arrived = lax.all_to_all(pieces, rows_axes, split_axis=0, concat_axis=0, tiled=True)
        arrived = arrived.reshape(groups, TEAM, depth, source.shape[1])
        return swap_add(jnp.sum(arrived.astype(F32), axis=0))

    expander_share = to_owners(expander_grad.astype(BF16))
    expander_out = (
        expander_share.reshape(TEAM, depth, groups, inner).transpose(1, 2, 0, 3).reshape(depth, FF)
    )
    reducer_pieces = lax.all_to_all(
        reducer_grad.astype(BF16).reshape(groups, inner, D),
        "grp",
        split_axis=0,
        concat_axis=0,
        tiled=True,
    )
    reducer_out = swap_add(jnp.sum(reducer_pieces.astype(F32), axis=0))
    combiner_low = combiner_grad.reshape(HEADS, LANES, D)[:, :HD].astype(BF16)
    if whole_heads:
        combiner_pieces = lax.all_to_all(
            combiner_low, "grp", split_axis=0, concat_axis=0, tiled=True
        )
        combiner_share = jnp.sum(combiner_pieces.astype(F32), axis=0)
    else:
        placed = jnp.zeros((HEADS, TEAM, HD, D), F32)
        placed = lax.dynamic_update_slice_in_dim(
            placed, combiner_low.astype(F32)[:, None], place, 1
        )
        combiner_share = lax.psum_scatter(
            placed.reshape(D, D), rows_axes, scatter_dimension=0, tiled=True
        )
    combiner_out = swap_add(combiner_share)
    projector_low = projector_grad.astype(BF16)
    project_share = to_owners(
        jnp.concatenate(
            [
                projector_low[:, : 3 * WIDE].reshape(D, 3 * HEADS, LANES)[:, :, :HD].reshape(
                    D, 3 * HEADS * HD
                ),
                projector_low[:, 3 * WIDE : 3 * WIDE + HEADS],
            ],
            axis=1,
        )
    )
    projector_out = (
        project_share[:, :, : 3 * HEADS * HD]
        .reshape(TEAM, depth, 3, HEADS, HD)
        .transpose(1, 2, 3, 0, 4)
        .reshape(depth, 3 * D)
    )
    forgetter_out = project_share[:, :, 3 * HEADS * HD :].transpose(1, 2, 0).reshape(depth, H)

    modulation_grad = jnp.concatenate(
        [
            shift_one_grad,
            scale_one_grad,
            gate_one_grad,
            shift_two_grad,
            scale_two_grad,
            gate_two_grad,
        ]
    ).reshape(devices, columns)
    modulation_rows = jnp.sum(
        lax.all_to_all(
            modulation_grad, rows_axes, split_axis=0, concat_axis=0, tiled=True
        ).reshape(groups, TEAM, columns),
        axis=1,
    )
    rows_every = lax.all_gather(modulation_rows, "items", axis=0, tiled=True)
    squashed_every = lax.all_gather(squashed, "items", axis=0, tiled=True).astype(F32)
    modulator_out = lax.dot_general(
        squashed_every, rows_every, (((0,), (0,)), ((), ())), precision=HIGH
    )
    baseline_out = jnp.sum(rows_every, axis=0)
    squashed_grad = jnp.dot(modulation_rows, modulator.astype(F32).T, precision=HIGH)

    def spot(value, shape, axis, at):
        return lax.dynamic_update_slice_in_dim(
            jnp.zeros(shape, F32), jnp.expand_dims(value, axis), at, axis
        ).reshape(-1)

    parts = [
        spot(squashed_grad, (halves, groups, D), 0, half),
        spot(retention_grad, (HEADS, TEAM), 1, place),
        spot(
            tap_stack.reshape(9, HEADS, LANES)[:, :, :HD], (9, HEADS, TEAM, HD), 2, place
        ),
        spot(pedestal_grad.reshape(HEADS, LANES)[:, :HD], (HEADS, TEAM, HD), 1, place),
        displacement_grad,
        spot(thresholds_grad.reshape(groups, inner), (groups, TEAM, inner), 1, place),
        leveling_grad,
    ]
    total = lax.psum(jnp.concatenate(parts), ("items", "grp", "pos"))
    split = []
    start = 0
    for part in parts:
        split.append(total[start : start + part.shape[0]])
        start += part.shape[0]
    squashed_sum = pick(split[0].reshape(halves, groups, D), 0, half)
    silu_pull = jax.vjp(jax.nn.silu, condition_float)[1]
    condition_grad = silu_pull(squashed_sum)[0]
    return (
        block_output,
        patches_grad,
        condition_grad,
        modulator_out,
        baseline_out,
        projector_out,
        forgetter_out,
        split[1],
        split[2].reshape(9, D),
        split[3],
        combiner_out,
        split[4],
        expander_out,
        split[5],
        reducer_out,
        split[6],
    )


def solution(mesh):
    rows = mesh.shape["rows"]
    groups = rows // TEAM
    fine = Mesh(
        mesh.devices.reshape(mesh.shape["items"], groups, TEAM), ("items", "grp", "pos")
    )
    line = ("grp", "pos")
    tokens = P(("items", "grp", "pos"), None, None)
    in_specs = (
        tokens,
        P("items", None),
        P("items"),
        P(None, line),
        P(line),
        P(line, None),
        P(line, None),
        P(),
        P(),
        P(),
        P(line, None),
        P(),
        P(line, None),
        P(),
        P(line, None),
        P(),
        tokens,
    )
    out_specs = (
        tokens,
        tokens,
        P("items", None),
        P(None, line),
        P(line),
        P(line, None),
        P(line, None),
        P(),
        P(),
        P(),
        P(line, None),
        P(),
        P(line, None),
        P(),
        P(line, None),
        P(),
    )
    return jax.shard_map(
        functools.partial(on_device, groups),
        mesh=fine,
        in_specs=in_specs,
        out_specs=out_specs,
        check_vma=False,
    )
```

```python
import functools

import jax
import jax.numpy as jnp
from jax import lax
from jax.experimental import pallas as pl
from jax.experimental.pallas import tpu as pltpu
from jax.sharding import Mesh, PartitionSpec as P

H = 16
HD = 72
D = 1152
FF = 4608
GRID = 32
PATCHES = 1024
ROWS_DEV = 4
TOK_DEV = 128
TEAM = GRID // ROWS_DEV
HEADS = H // TEAM
LANES = 128
WIDE = HEADS * LANES
STRIP = 256

EPS = 1e-06
HIGH = lax.Precision.HIGHEST
F32 = jnp.float32
BF16 = jnp.bfloat16
FACTOR = HD ** (-0.5)


def modulate(values, offset, stretch):
    centred = values - jnp.mean(values, axis=-1, keepdims=True)
    spread = jnp.mean(centred * centred, axis=-1, keepdims=True)
    return centred * lax.rsqrt(spread + EPS) * (1.0 + stretch) + offset


def dot(left, right):
    return jnp.dot(left, right, preferred_element_type=F32)


def outer_sum(left, right):
    return lax.dot_general(left, right, (((0,), (0,)), ((), ())), preferred_element_type=F32)


def back_dot(gradient, matrix):
    return lax.dot_general(gradient, matrix, (((1,), (1,)), ((), ())), preferred_element_type=F32)


def column_place(index):
    return (index & (GRID - 1)) * GRID + (index >> 5)


def strip_weights(start, gcol, grow):
    rows = lax.broadcasted_iota(jnp.int32, (STRIP, PATCHES), 0) + start
    cols = lax.broadcasted_iota(jnp.int32, (STRIP, PATCHES), 1)
    causal = column_place(cols) <= column_place(rows)
    return jnp.exp(jnp.where(causal, gcol - grow, -1e30))


def attend_kernel(q_ref, k_ref, v_ref, gcol_ref, grow_ref, out_ref):
    keys = k_ref[...]
    values = v_ref[...]
    grow = grow_ref[0]

    def strip(number, carry):
        start = pl.multiple_of(number * STRIP, STRIP)
        here = pl.ds(start, STRIP)
        weights = strip_weights(start, gcol_ref[0, here, :], grow)
        scores = back_dot(q_ref[here, :], keys) * weights
        out_ref[here, :] = (dot(scores.astype(BF16), values) * FACTOR).astype(BF16)
        return carry

    lax.fori_loop(0, PATCHES // STRIP, strip, 0)


def attend_back_kernel(
    q_ref, k_ref, v_ref, gcol_ref, grow_ref, do_ref, dq_ref, dk_ref, dv_ref, row_ref, col_ref
):
    keys = k_ref[...]
    values = v_ref[...]
    grow = grow_ref[0]
    dk_ref[...] = jnp.zeros_like(dk_ref)
    dv_ref[...] = jnp.zeros_like(dv_ref)
    col_ref[...] = jnp.zeros_like(col_ref)

    def strip(number, carry):
        start = pl.multiple_of(number * STRIP, STRIP)
        here = pl.ds(start, STRIP)
        queries = q_ref[here, :]
        grads = do_ref[here, :]
        weights = strip_weights(start, gcol_ref[0, here, :], grow)
        scores = back_dot(queries, keys) * weights
        back = back_dot(grads, values)
        pulled = (back * weights).astype(BF16)
        moment = back * scores
        dv_ref[...] += outer_sum(scores.astype(BF16), grads)
        dk_ref[...] += outer_sum(pulled, queries)
        dq_ref[here, :] = dot(pulled, keys) * FACTOR
        row_ref[0, here, :] = jnp.sum(moment, axis=1, keepdims=True) * FACTOR
        col_ref[0] += jnp.sum(moment, axis=0, keepdims=True) * FACTOR
        return carry

    lax.fori_loop(0, PATCHES // STRIP, strip, 0)
    dk_ref[...] *= FACTOR
    dv_ref[...] *= FACTOR


def head_specs():
    return [
        pl.BlockSpec((PATCHES, LANES), lambda h: (0, h)),
        pl.BlockSpec((PATCHES, LANES), lambda h: (0, HEADS + h)),
        pl.BlockSpec((PATCHES, LANES), lambda h: (0, 2 * HEADS + h)),
        pl.BlockSpec((1, PATCHES, 1), lambda h: (h, 0, 0)),
        pl.BlockSpec((1, 1, PATCHES), lambda h: (h, 0, 0)),
    ]


def attend(qkv, gcol, grow):
    return pl.pallas_call(
        attend_kernel,
        grid=(HEADS,),
        out_shape=jax.ShapeDtypeStruct((PATCHES, WIDE), BF16),
        in_specs=head_specs(),
        out_specs=pl.BlockSpec((PATCHES, LANES), lambda h: (0, h)),
        cost_estimate=pl.CostEstimate(
            flops=HEADS * 4 * PATCHES * PATCHES * LANES,
            bytes_accessed=8 * PATCHES * WIDE,
            transcendentals=HEADS * PATCHES * PATCHES,
        ),
        name="attend",
    )(qkv, qkv, qkv, gcol, grow)


def attend_back(qkv, gcol, grow, grads):
    block = pl.BlockSpec((PATCHES, LANES), lambda h: (0, h))
    return pl.pallas_call(
        attend_back_kernel,
        grid=(HEADS,),
        out_shape=[jax.ShapeDtypeStruct((PATCHES, WIDE), F32)] * 3
        + [
            jax.ShapeDtypeStruct((HEADS, PATCHES, 1), F32),
            jax.ShapeDtypeStruct((HEADS, 1, PATCHES), F32),
        ],
        in_specs=head_specs() + [block],
        out_specs=[block, block, block]
        + [
            pl.BlockSpec((1, PATCHES, 1), lambda h: (h, 0, 0)),
            pl.BlockSpec((1, 1, PATCHES), lambda h: (h, 0, 0)),
        ],
        cost_estimate=pl.CostEstimate(
            flops=HEADS * 10 * PATCHES * PATCHES * LANES,
            bytes_accessed=20 * PATCHES * WIDE,
            transcendentals=HEADS * PATCHES * PATCHES,
        ),
        name="attend_back",
    )(qkv, qkv, qkv, gcol, grow, grads)


def pad_heads(source, axis):
    widths = [(0, 0)] * source.ndim
    widths[axis] = (0, LANES - HD)
    return jnp.pad(source, widths)


def pad_cells(grid):
    return jnp.pad(grid, ((1, 1), (1, 1), (0, 0)))


def pick(source, axis, index):
    return lax.dynamic_index_in_dim(source, index, axis, keepdims=False)


MESH = pl.DeviceIdType.MESH


def greet(peers):
    barrier = pltpu.get_barrier_semaphore()
    for peer in peers:
        pl.semaphore_signal(barrier, inc=1, device_id=peer, device_id_type=MESH)
    pl.semaphore_wait(barrier, len(peers))


def team_peers():
    place = lax.axis_index("pos")
    up, side, core = place // 4, (place // 2) % 2, place % 2
    return up, side, core


def seat(up, side, core):
    return up * 4 + side * 2 + core


def team_gather_kernel(x_ref, out_ref, send_sem, recv_sem):
    up, side, core = team_peers()
    mine = seat(up, side, core)
    above, beside, across = (
        seat(1 - up, side, core),
        seat(up, 1 - side, core),
        seat(1 - up, 1 - side, core),
    )
    twin = {"pos": seat(up, side, 1 - core)}
    to_up = {"pos": above}
    to_side = {"pos": beside}
    greet((to_up, to_side, twin))
    rows = x_ref.shape[0]
    parts = (pl.ds(0, rows // 2), pl.ds(rows // 2, rows // 2))

    def send(slot, source, owner, part, peer):
        copy = pltpu.make_async_remote_copy(
            src_ref=source,
            dst_ref=out_ref.at[owner, part],
            send_sem=send_sem.at[slot],
            recv_sem=recv_sem.at[slot],
            device_id=peer,
            device_id_type=MESH,
        )
        copy.start()
        return copy

    held = [
        send(0, x_ref.at[parts[0]], mine, parts[0], to_up),
        send(1, x_ref.at[parts[1]], mine, parts[1], to_side),
        send(2, x_ref.at[parts[1]], mine, parts[1], to_up),
        send(3, x_ref.at[parts[0]], mine, parts[0], to_side),
        send(4, x_ref.at[parts[0]], mine, parts[0], twin),
        send(5, x_ref.at[parts[1]], mine, parts[1], twin),
    ]
    out_ref[mine] = x_ref[...]
    held[0].wait_recv()
    held.append(send(6, out_ref.at[above, parts[0]], above, parts[0], to_side))
    held.append(send(7, out_ref.at[above, parts[0]], above, parts[0], twin))
    held[1].wait_recv()
    held.append(send(8, out_ref.at[beside, parts[1]], beside, parts[1], to_up))
    held.append(send(9, out_ref.at[beside, parts[1]], beside, parts[1], twin))
    held[2].wait_recv()
    held.append(send(10, out_ref.at[above, parts[1]], above, parts[1], twin))
    held[3].wait_recv()
    held.append(send(11, out_ref.at[beside, parts[0]], beside, parts[0], twin))
    held[6].wait_recv()
    held.append(send(12, out_ref.at[across, parts[0]], across, parts[0], twin))
    held[8].wait_recv()
    held.append(send(13, out_ref.at[across, parts[1]], across, parts[1], twin))
    for slot in (4, 5, 7, 9, 10, 11, 12, 13):
        held[slot].wait_recv()
    for copy in held:
        copy.wait_send()


def team_gather(source):
    rows, width = source.shape
    vmem = pl.BlockSpec(memory_space=pltpu.VMEM)
    return pl.pallas_call(
        team_gather_kernel,
        out_shape=jax.ShapeDtypeStruct((TEAM, rows, width), source.dtype),
        in_specs=[vmem],
        out_specs=vmem,
        scratch_shapes=[pltpu.SemaphoreType.DMA((14,)), pltpu.SemaphoreType.DMA((14,))],
        compiler_params=pltpu.CompilerParams(collective_id=1, has_side_effects=True),
        name="team_gather",
    )(source).reshape(TEAM * rows, width)


def team_scatter_kernel(x_ref, out_ref, twins, low, first, turned, second, send_sem, recv_sem):
    up, side, core = team_peers()
    twin = {"pos": seat(up, side, 1 - core)}
    to_up = {"pos": seat(1 - up, side, core)}
    to_side = {"pos": seat(up, 1 - side, core)}
    greet((to_up, to_side, twin))
    rows = x_ref.shape[1]
    part_rows = rows // 2
    parts = (pl.ds(0, part_rows), pl.ds(part_rows, part_rows))

    def send(slot, source, target, peer):
        copy = pltpu.make_async_remote_copy(
            src_ref=source,
            dst_ref=target,
            send_sem=send_sem.at[slot],
            recv_sem=recv_sem.at[slot],
            device_id=peer,
            device_id_type=MESH,
        )
        copy.start()
        return copy

    chips = ((1 - up, 1 - side), (1 - up, side), (up, 1 - side), (up, side))
    held = []
    for slot, (u, s) in enumerate(chips):
        held.append(send(slot, x_ref.at[seat(u, s, 1 - core)], twins.at[u * 2 + s], twin))

    def merge(slot):
        u, s = chips[slot]
        held[slot].wait_recv()
        low[u * 2 + s] = (
            x_ref[seat(u, s, core)].astype(F32) + twins[u * 2 + s].astype(F32)
        ).astype(BF16)

    merge(0)
    a_far = send(4, low.at[(1 - up) * 2 + 1 - side, parts[0]], first.at[1 - side], to_up)
    b_far = send(5, low.at[(1 - up) * 2 + 1 - side, parts[1]], first.at[2 + 1 - up], to_side)
    merge(1)
    a_near = send(6, low.at[(1 - up) * 2 + side, parts[0]], first.at[side], to_up)
    merge(2)
    b_near = send(7, low.at[up * 2 + 1 - side, parts[1]], first.at[2 + up], to_side)
    merge(3)
    a_far.wait_recv()
    turned[0] = (
        low[up * 2 + 1 - side, parts[0]].astype(F32) + first[1 - side].astype(F32)
    ).astype(BF16)
    a_last = send(8, turned.at[0], second.at[0], to_side)
    b_far.wait_recv()
    turned[1] = (
        low[(1 - up) * 2 + side, parts[1]].astype(F32) + first[2 + 1 - up].astype(F32)
    ).astype(BF16)
    b_last = send(9, turned.at[1], second.at[1], to_up)
    a_near.wait_recv()
    b_near.wait_recv()
    a_last.wait_recv()
    out_ref[parts[0]] = (
        low[up * 2 + side, parts[0]].astype(F32)
        + first[side].astype(F32)
        + second[0].astype(F32)
    )
    b_last.wait_recv()
    out_ref[parts[1]] = (
        low[up * 2 + side, parts[1]].astype(F32)
        + first[2 + up].astype(F32)
        + second[1].astype(F32)
    )
    for copy in held + [a_far, b_far, a_near, b_near, a_last, b_last]:
        copy.wait_send()


def team_scatter(partial):
    rows, width = partial.shape[0] // TEAM, partial.shape[1]
    vmem = pl.BlockSpec(memory_space=pltpu.VMEM)
    return pl.pallas_call(
        team_scatter_kernel,
        out_shape=jax.ShapeDtypeStruct((rows, width), F32),
        in_specs=[vmem],
        out_specs=vmem,
        scratch_shapes=[
            pltpu.VMEM((4, rows, width), BF16),
            pltpu.VMEM((4, rows, width), BF16),
            pltpu.VMEM((4, rows // 2, width), BF16),
            pltpu.VMEM((2, rows // 2, width), BF16),
            pltpu.VMEM((2, rows // 2, width), BF16),
            pltpu.SemaphoreType.DMA((10,)),
            pltpu.SemaphoreType.DMA((10,)),
        ],
        compiler_params=pltpu.CompilerParams(collective_id=2, has_side_effects=True),
        name="team_scatter",
    )(partial.astype(BF16).reshape(TEAM, rows, width))


def flat_peer(index, sizes):
    halves, groups = sizes
    where = {"grp": (index // TEAM) % groups, "pos": index % TEAM}
    if halves > 1:
        where["items"] = index // (TEAM * groups)
    return where


def flat_index(sizes):
    halves, groups = sizes
    here = lax.axis_index("grp") * TEAM + lax.axis_index("pos")
    if halves > 1:
        here = here + lax.axis_index("items") * (TEAM * groups)
    return here


def greet_all(me, total, sizes):
    barrier = pltpu.get_barrier_semaphore()

    def call(step, carry):
        pl.semaphore_signal(
            barrier,
            inc=1,
            device_id=flat_peer((me + step) % total, sizes),
            device_id_type=MESH,
        )
        return carry

    lax.fori_loop(1, total, call, 0)
    pl.semaphore_wait(barrier, total - 1)


def send_all(me, total, sizes, source_of, target, send_sem, recv_sem, whole):
    def describe(step):
        peer = (me + step) % total
        return pltpu.make_async_remote_copy(
            src_ref=source_of(peer),
            dst_ref=target,
            send_sem=send_sem,
            recv_sem=recv_sem,
            device_id=flat_peer(peer, sizes),
            device_id_type=MESH,
        )

    def start(step, carry):
        describe(step).start()
        return carry

    lax.fori_loop(1, total, start, 0)
    everything = pltpu.make_async_remote_copy(
        src_ref=whole.at[pl.ds(0, total - 1)],
        dst_ref=whole.at[pl.ds(0, total - 1)],
        send_sem=send_sem,
        recv_sem=recv_sem,
        device_id=flat_peer((me + 1) % total, sizes),
        device_id_type=MESH,
    )
    everything.wait_recv()
    everything.wait_send()


def small_gather_kernel(sizes, x_ref, out_ref, send_sem, recv_sem):
    total = sizes[0] * sizes[1] * TEAM
    me = flat_index(sizes)
    greet_all(me, total, sizes)
    out_ref[me] = x_ref[...]
    send_all(me, total, sizes, lambda peer: x_ref, out_ref.at[me], send_sem, recv_sem, out_ref)


def small_gather(source, sizes, number):
    total = sizes[0] * sizes[1] * TEAM
    count = source.shape[0]
    lines = -(-count // 1024) * 8
    padded = jnp.pad(source, (0, lines * 128 - count)).reshape(lines, 128)
    vmem = pl.BlockSpec(memory_space=pltpu.VMEM)
    out = pl.pallas_call(
        functools.partial(small_gather_kernel, sizes),
        out_shape=jax.ShapeDtypeStruct((total, lines, 128), F32),
        in_specs=[vmem],
        out_specs=vmem,
        scratch_shapes=[pltpu.SemaphoreType.DMA, pltpu.SemaphoreType.DMA],
        compiler_params=pltpu.CompilerParams(collective_id=number, has_side_effects=True),
        name="small_gather",
    )(padded)
    return out.reshape(total, lines * 128)[:, :count]


def small_sum_kernel(sizes, x_ref, out_ref, came, summed, sems):
    total = sizes[0] * sizes[1] * TEAM
    me = flat_index(sizes)
    greet_all(me, total, sizes)
    came[me] = x_ref[me]
    send_all(
        me, total, sizes, lambda peer: x_ref.at[peer], came.at[me], sems.at[0], sems.at[1], came
    )
    result = jnp.sum(came[...], axis=0)
    summed[...] = result
    out_ref[me] = result
    send_all(
        me, total, sizes, lambda peer: summed, out_ref.at[me], sems.at[2], sems.at[3], out_ref
    )


def small_sum(source, sizes, number):
    total = sizes[0] * sizes[1] * TEAM
    count = source.shape[0]
    lines = -(-count // (1024 * total)) * 8
    padded = jnp.pad(source, (0, total * lines * 128 - count)).reshape(total, lines, 128)
    vmem = pl.BlockSpec(memory_space=pltpu.VMEM)
    out = pl.pallas_call(
        functools.partial(small_sum_kernel, sizes),
        out_shape=jax.ShapeDtypeStruct((total, lines, 128), F32),
        in_specs=[vmem],
        out_specs=vmem,
        scratch_shapes=[
            pltpu.VMEM((total, lines, 128), F32),
            pltpu.VMEM((lines, 128), F32),
            pltpu.SemaphoreType.DMA((4,)),
        ],
        compiler_params=pltpu.CompilerParams(collective_id=number, has_side_effects=True),
        name="small_sum",
    )(padded)
    return out.reshape(-1)[:count]


def on_device(
    groups,
    patches,
    condition,
    lengths,
    modulator,
    baseline,
    projector,
    forgetter,
    retention,
    smoother,
    pedestal,
    combiner,
    displacement,
    expander,
    thresholds,
    reducer,
    leveling,
    cotangent,
):
    rows_axes = ("grp", "pos")
    half = lax.axis_index("items")
    halves = lax.axis_size("items")
    group = lax.axis_index("grp")
    place = lax.axis_index("pos")
    devices = groups * TEAM
    depth = D // devices
    inner = FF // devices
    columns = 6 * D // devices
    whole_heads = depth == HD
    upstream = cotangent.astype(F32).reshape(TOK_DEV, D)
    inputs = patches.astype(F32).reshape(TOK_DEV, D)

    condition_float = condition.astype(F32)
    squashed = jax.nn.silu(condition_float).astype(BF16)
    modulation_piece = (dot(squashed, modulator) + baseline).astype(BF16).T
    modulation_all = small_gather(
        modulation_piece.T.astype(F32).reshape(-1), (1, groups), 3
    ).reshape(devices, groups, columns)
    modulation = pick(modulation_all, 1, group).reshape(-1)
    shift_one, scale_one, gate_one, shift_two, scale_two, gate_two = [
        modulation[part * D : (part + 1) * D] for part in range(6)
    ]

    def group_gather(source):
        if groups != 2:
            return lax.all_gather(source, "grp", axis=0, tiled=True)
        other = lax.ppermute(source, "grp", [(0, 1), (1, 0)])
        first = group == 0
        return jnp.concatenate(
            [jnp.where(first, source, other), jnp.where(first, other, source)], axis=0
        )

    project_cut = jnp.concatenate(
        [
            projector.reshape(depth, 3, HEADS, TEAM, HD)
            .transpose(3, 0, 1, 2, 4)
            .reshape(TEAM, depth, 3 * HEADS * HD),
            forgetter.reshape(depth, HEADS, TEAM).transpose(2, 0, 1),
        ],
        axis=2,
    )
    project_part = lax.all_to_all(project_cut, "pos", split_axis=0, concat_axis=0, tiled=True)
    project_mine = group_gather(project_part).reshape(D, -1)
    project_wide = jnp.concatenate(
        [
            pad_heads(project_mine[:, : 3 * HEADS * HD].reshape(D, 3 * HEADS, HD), 2).reshape(
                D, 3 * WIDE
            ),
            jnp.pad(project_mine[:, 3 * HEADS * HD :], ((0, 0), (0, LANES - HEADS))),
        ],
        axis=1,
    )
    expand_cut = (
        expander.reshape(depth, groups, TEAM, inner)
        .transpose(2, 0, 1, 3)
        .reshape(TEAM, depth, groups * inner)
    )
    expand_part = lax.all_to_all(expand_cut, "pos", split_axis=0, concat_axis=0, tiled=True)
    expand_mine = group_gather(expand_part).reshape(D, groups * inner)
    reduce_mine = group_gather(reducer)
    if whole_heads:
        combine_mine = group_gather(combiner).reshape(HEADS, HD, D)
    else:
        combine_all = lax.all_gather(combiner, rows_axes, axis=0, tiled=True)
        combine_mine = pick(combine_all.reshape(HEADS, TEAM, HD, D), 1, place)
    combine_wide = pad_heads(combine_mine, 1).reshape(WIDE, D)
    thresholds_mine = pick(thresholds.reshape(groups, TEAM, inner), 1, place).reshape(-1)
    retention_mine = pick(retention.reshape(HEADS, TEAM), 1, place)
    kernel = pad_heads(pick(smoother.reshape(9, HEADS, TEAM, HD), 2, place), 2).reshape(9, WIDE)
    offset = pad_heads(pick(pedestal.reshape(HEADS, TEAM, HD), 1, place), 1).reshape(WIDE)

    hidden = modulate(inputs, shift_one, scale_one).astype(BF16)
    hidden_all = team_gather(hidden)
    projected = dot(hidden_all, project_wide)
    forget_logit = projected[:, 3 * WIDE : 3 * WIDE + HEADS] + retention_mine
    decays = (jax.nn.log_sigmoid(forget_logit) / 16.0).astype(BF16)
    index = jnp.arange(PATCHES, dtype=jnp.int32)
    length = pick(lengths, 0, group)
    validity = (index < length)[:, None]
    is_query = jnp.arange(3 * WIDE) < WIDE
    keep = validity | is_query[None, :]
    qkv = jnp.where(keep, projected[:, : 3 * WIDE], 0.0).astype(BF16)
    order = column_place(index)
    causal = (order[None, :] <= order[:, None]).astype(BF16)
    summed = dot(causal, decays)
    gcol = summed.T[:, :, None]
    grow = summed.T[:, None, :]
    attended = attend(qkv, gcol, grow)

    attended_grid = attended.astype(F32).reshape(GRID, GRID, WIDE)
    attended_padded = pad_cells(attended_grid)
    smoothed = jnp.zeros_like(attended_grid) + offset
    for tap in range(9):
        down, right = tap // 3, tap % 3
        smoothed = (
            smoothed + kernel[tap] * attended_padded[down : down + GRID, right : right + GRID]
        )
    smoothed = smoothed.astype(BF16).reshape(PATCHES, WIDE)
    branch = team_scatter(dot(smoothed, combine_wide)) + displacement
    middle = inputs + gate_one * branch
    hidden_two = modulate(middle, shift_two, scale_two).astype(BF16)
    hidden_two_all = team_gather(hidden_two)
    expanded = dot(hidden_two_all, expand_mine) + thresholds_mine
    activated = jax.nn.gelu(expanded, approximate=True).astype(BF16)
    reduced = team_scatter(dot(activated, reduce_mine)) + leveling
    block_output = (middle + gate_two * reduced).astype(BF16).reshape(ROWS_DEV, GRID, D)

    gate_two_grad = jnp.sum(upstream * reduced, axis=0)
    reduced_grad = (gate_two * upstream).astype(BF16)
    leveling_grad = jnp.sum(reduced_grad.astype(F32), axis=0)
    reduced_grad_all = team_gather(reduced_grad)
    reducer_grad = outer_sum(activated, reduced_grad_all)
    activated_grad = back_dot(reduced_grad_all, reduce_mine)
    pull = jax.vjp(lambda v: jax.nn.gelu(v, approximate=True), expanded)[1]
    expanded_grad = pull(activated_grad)[0].astype(BF16)
    thresholds_grad = jnp.sum(expanded_grad.astype(F32), axis=0)
    expander_grad = outer_sum(hidden_two_all, expanded_grad)
    hidden_two_grad = team_scatter(back_dot(expanded_grad, expand_mine))
    second_pull = jax.vjp(modulate, middle, shift_two, scale_two)[1]
    middle_part, shift_two_grad, scale_two_grad = second_pull(hidden_two_grad)
    middle_grad = upstream + middle_part
    gate_one_grad = jnp.sum(middle_grad * branch, axis=0)
    branch_grad = (gate_one * middle_grad).astype(BF16)
    displacement_grad = jnp.sum(branch_grad.astype(F32), axis=0)
    branch_grad_all = team_gather(branch_grad)
    combiner_grad = outer_sum(smoothed, branch_grad_all)
    smoothed_grad = back_dot(branch_grad_all, combine_wide).astype(BF16).astype(F32)
    pedestal_grad = jnp.sum(smoothed_grad, axis=0)
    grad_grid = smoothed_grad.reshape(GRID, GRID, WIDE)
    grad_padded = pad_cells(grad_grid)
    tap_grads = []
    attended_grad = jnp.zeros_like(grad_grid)
    for tap in range(9):
        down, right = tap // 3, tap % 3
        tap_grads.append(
            jnp.sum(
                grad_grid * attended_padded[down : down + GRID, right : right + GRID], axis=(0, 1)
            )
        )
        attended_grad = (
            attended_grad
            + kernel[tap] * grad_padded[2 - down : 2 - down + GRID, 2 - right : 2 - right + GRID]
        )
    tap_stack = jnp.stack(tap_grads)
    attended_grad = attended_grad.astype(BF16).reshape(PATCHES, WIDE)
    dq, dk, dv, row_sum, col_sum = attend_back(qkv, gcol, grow, attended_grad)
    moment = row_sum[:, :, 0] - col_sum[:, 0, :]
    decay_grad = lax.dot_general(
        causal.astype(F32),
        moment,
        (((0,), (1,)), ((), ())),
        precision=HIGH,
        preferred_element_type=F32,
    )
    forget_grad = (decay_grad * jax.nn.sigmoid(-forget_logit) / 16.0).astype(BF16)
    retention_grad = jnp.sum(forget_grad.astype(F32), axis=0)
    project_grad = jnp.concatenate(
        [
            dq.astype(BF16),
            jnp.where(validity, dk, 0.0).astype(BF16),
            jnp.where(validity, dv, 0.0).astype(BF16),
            jnp.pad(forget_grad, ((0, 0), (0, LANES - HEADS))),
        ],
        axis=1,
    )
    projector_grad = outer_sum(hidden_all, project_grad)
    hidden_grad = team_scatter(back_dot(project_grad, project_wide))
    first_pull = jax.vjp(modulate, inputs, shift_one, scale_one)[1]
    inputs_part, shift_one_grad, scale_one_grad = first_pull(hidden_grad)
    patches_grad = (middle_grad + inputs_part).astype(BF16).reshape(ROWS_DEV, GRID, D)

    def swap_add(share):
        low = share.astype(BF16)
        other = lax.ppermute(low, "items", [(i, (i + 1) % 2) for i in range(2)])
        return low.astype(F32) + other.astype(F32)

    def to_owners(source):
        pieces = source.reshape(devices, depth, source.shape[1])
        arrived = lax.all_to_all(pieces, rows_axes, split_axis=0, concat_axis=0, tiled=True)
        arrived = arrived.reshape(groups, TEAM, depth, source.shape[1])
        return swap_add(jnp.sum(arrived.astype(F32), axis=0))

    expander_share = to_owners(expander_grad.astype(BF16))
    expander_out = (
        expander_share.reshape(TEAM, depth, groups, inner).transpose(1, 2, 0, 3).reshape(depth, FF)
    )
    reducer_pieces = lax.all_to_all(
        reducer_grad.astype(BF16).reshape(groups, inner, D),
        "grp",
        split_axis=0,
        concat_axis=0,
        tiled=True,
    )
    reducer_out = swap_add(jnp.sum(reducer_pieces.astype(F32), axis=0))
    combiner_low = combiner_grad.reshape(HEADS, LANES, D)[:, :HD].astype(BF16)
    if whole_heads:
        combiner_pieces = lax.all_to_all(
            combiner_low, "grp", split_axis=0, concat_axis=0, tiled=True
        )
        combiner_share = jnp.sum(combiner_pieces.astype(F32), axis=0)
    else:
        placed = jnp.zeros((HEADS, TEAM, HD, D), F32)
        placed = lax.dynamic_update_slice_in_dim(
            placed, combiner_low.astype(F32)[:, None], place, 1
        )
        combiner_share = lax.psum_scatter(
            placed.reshape(D, D), rows_axes, scatter_dimension=0, tiled=True
        )
    combiner_out = swap_add(combiner_share)
    projector_low = projector_grad.astype(BF16)
    project_share = to_owners(
        jnp.concatenate(
            [
                projector_low[:, : 3 * WIDE].reshape(D, 3 * HEADS, LANES)[:, :, :HD].reshape(
                    D, 3 * HEADS * HD
                ),
                projector_low[:, 3 * WIDE : 3 * WIDE + HEADS],
            ],
            axis=1,
        )
    )
    projector_out = (
        project_share[:, :, : 3 * HEADS * HD]
        .reshape(TEAM, depth, 3, HEADS, HD)
        .transpose(1, 2, 3, 0, 4)
        .reshape(depth, 3 * D)
    )
    forgetter_out = project_share[:, :, 3 * HEADS * HD :].transpose(1, 2, 0).reshape(depth, H)

    def spot(value, shape, axis, at):
        return lax.dynamic_update_slice_in_dim(
            jnp.zeros(shape, F32), jnp.expand_dims(value, axis), at, axis
        ).reshape(-1)

    def sum_everywhere(parts, number):
        total = small_sum(jnp.concatenate(parts), (halves, groups), number)
        split = []
        start = 0
        for part in parts:
            split.append(total[start : start + part.shape[0]])
            start += part.shape[0]
        return split

    modulation_grad = jnp.concatenate(
        [
            shift_one_grad,
            scale_one_grad,
            gate_one_grad,
            shift_two_grad,
            scale_two_grad,
            gate_two_grad,
        ]
    )
    item = half * groups + group
    here = ((group == 0) & (place == 0)).astype(F32)
    split = sum_everywhere(
        [
            spot(modulation_grad, (halves * groups, 6 * D), 0, item),
            spot(retention_grad, (HEADS, TEAM), 1, place),
            spot(
                tap_stack.reshape(9, HEADS, LANES)[:, :, :HD], (9, HEADS, TEAM, HD), 2, place
            ),
            spot(pedestal_grad.reshape(HEADS, LANES)[:, :HD], (HEADS, TEAM, HD), 1, place),
            displacement_grad,
            spot(thresholds_grad.reshape(groups, inner), (groups, TEAM, inner), 1, place),
            leveling_grad,
            spot(squashed.astype(F32) * here, (halves, groups, D), 0, half),
        ],
        4,
    )
    device = group * TEAM + place
    rows_every = pick(split[0].reshape(halves * groups, devices, columns), 1, device)
    squashed_every = split[7].reshape(halves * groups, D)
    modulator_out = lax.dot_general(
        squashed_every, rows_every, (((0,), (0,)), ((), ())), precision=HIGH
    )
    baseline_out = jnp.sum(rows_every, axis=0)
    modulation_rows = pick(rows_every.reshape(halves, groups, columns), 0, half)
    squashed_grad = jnp.dot(modulation_rows, modulator.astype(F32).T, precision=HIGH)
    squashed_total = sum_everywhere(
        [spot(squashed_grad, (halves, groups, D), 0, half)], 5
    )[0]
    squashed_sum = pick(squashed_total.reshape(halves, groups, D), 0, half)
    silu_pull = jax.vjp(jax.nn.silu, condition_float)[1]
    condition_grad = silu_pull(squashed_sum)[0]
    return (
        block_output,
        patches_grad,
        condition_grad,
        modulator_out,
        baseline_out,
        projector_out,
        forgetter_out,
        split[1],
        split[2].reshape(9, D),
        split[3],
        combiner_out,
        split[4],
        expander_out,
        split[5],
        reducer_out,
        split[6],
    )


def solution(mesh):
    rows = mesh.shape["rows"]
    groups = rows // TEAM
    fine = Mesh(
        mesh.devices.reshape(mesh.shape["items"], groups, TEAM), ("items", "grp", "pos")
    )
    line = ("grp", "pos")
    tokens = P(("items", "grp", "pos"), None, None)
    in_specs = (
        tokens,
        P("items", None),
        P("items"),
        P(None, line),
        P(line),
        P(line, None),
        P(line, None),
        P(),
        P(),
        P(),
        P(line, None),
        P(),
        P(line, None),
        P(),
        P(line, None),
        P(),
        tokens,
    )
    out_specs = (
        tokens,
        tokens,
        P("items", None),
        P(None, line),
        P(line),
        P(line, None),
        P(line, None),
        P(),
        P(),
        P(),
        P(line, None),
        P(),
        P(line, None),
        P(),
        P(line, None),
        P(),
    )
    return jax.shard_map(
        functools.partial(on_device, groups),
        mesh=fine,
        in_specs=in_specs,
        out_specs=out_specs,
        check_vma=False,
    )
```

```python
import functools

import jax
import jax.numpy as jnp
from jax import lax
from jax.experimental import pallas as pl
from jax.experimental.pallas import tpu as pltpu
from jax.sharding import Mesh, PartitionSpec as P

H = 16
HD = 72
D = 1152
FF = 4608
GRID = 32
PATCHES = 1024
ROWS_DEV = 4
TOK_DEV = 128
TEAM = GRID // ROWS_DEV
HEADS = H // TEAM
LANES = 128
WIDE = HEADS * LANES
STRIP = 256

EPS = 1e-06
HIGH = lax.Precision.HIGHEST
F32 = jnp.float32
BF16 = jnp.bfloat16
FACTOR = HD ** (-0.5)


def modulate(values, offset, stretch):
    centred = values - jnp.mean(values, axis=-1, keepdims=True)
    spread = jnp.mean(centred * centred, axis=-1, keepdims=True)
    return centred * lax.rsqrt(spread + EPS) * (1.0 + stretch) + offset


def dot(left, right):
    return jnp.dot(left, right, preferred_element_type=F32)


def outer_sum(left, right):
    return lax.dot_general(left, right, (((0,), (0,)), ((), ())), preferred_element_type=F32)


def back_dot(gradient, matrix):
    return lax.dot_general(gradient, matrix, (((1,), (1,)), ((), ())), preferred_element_type=F32)


def column_place(index):
    return (index & (GRID - 1)) * GRID + (index >> 5)


def strip_weights(start, gcol, grow):
    rows = lax.broadcasted_iota(jnp.int32, (STRIP, PATCHES), 0) + start
    cols = lax.broadcasted_iota(jnp.int32, (STRIP, PATCHES), 1)
    causal = column_place(cols) <= column_place(rows)
    return jnp.exp(jnp.where(causal, gcol - grow, -1e30))


def attend_kernel(q_ref, k_ref, v_ref, gcol_ref, grow_ref, out_ref):
    keys = k_ref[...]
    values = v_ref[...]
    grow = grow_ref[0]

    def strip(number, carry):
        start = pl.multiple_of(number * STRIP, STRIP)
        here = pl.ds(start, STRIP)
        weights = strip_weights(start, gcol_ref[0, here, :], grow)
        scores = back_dot(q_ref[here, :], keys) * weights
        out_ref[here, :] = (dot(scores.astype(BF16), values) * FACTOR).astype(BF16)
        return carry

    lax.fori_loop(0, PATCHES // STRIP, strip, 0)


def attend_back_kernel(
    q_ref, k_ref, v_ref, gcol_ref, grow_ref, do_ref, dq_ref, dk_ref, dv_ref, row_ref, col_ref
):
    keys = k_ref[...]
    values = v_ref[...]
    grow = grow_ref[0]
    dk_ref[...] = jnp.zeros_like(dk_ref)
    dv_ref[...] = jnp.zeros_like(dv_ref)
    col_ref[...] = jnp.zeros_like(col_ref)

    def strip(number, carry):
        start = pl.multiple_of(number * STRIP, STRIP)
        here = pl.ds(start, STRIP)
        queries = q_ref[here, :]
        grads = do_ref[here, :]
        weights = strip_weights(start, gcol_ref[0, here, :], grow)
        scores = back_dot(queries, keys) * weights
        back = back_dot(grads, values)
        pulled = (back * weights).astype(BF16)
        moment = back * scores
        dv_ref[...] += outer_sum(scores.astype(BF16), grads)
        dk_ref[...] += outer_sum(pulled, queries)
        dq_ref[here, :] = dot(pulled, keys) * FACTOR
        row_ref[0, here, :] = jnp.sum(moment, axis=1, keepdims=True) * FACTOR
        col_ref[0] += jnp.sum(moment, axis=0, keepdims=True) * FACTOR
        return carry

    lax.fori_loop(0, PATCHES // STRIP, strip, 0)
    dk_ref[...] *= FACTOR
    dv_ref[...] *= FACTOR


def head_specs():
    return [
        pl.BlockSpec((PATCHES, LANES), lambda h: (0, h)),
        pl.BlockSpec((PATCHES, LANES), lambda h: (0, HEADS + h)),
        pl.BlockSpec((PATCHES, LANES), lambda h: (0, 2 * HEADS + h)),
        pl.BlockSpec((1, PATCHES, 1), lambda h: (h, 0, 0)),
        pl.BlockSpec((1, 1, PATCHES), lambda h: (h, 0, 0)),
    ]


def attend(qkv, gcol, grow):
    return pl.pallas_call(
        attend_kernel,
        grid=(HEADS,),
        out_shape=jax.ShapeDtypeStruct((PATCHES, WIDE), BF16),
        in_specs=head_specs(),
        out_specs=pl.BlockSpec((PATCHES, LANES), lambda h: (0, h)),
        cost_estimate=pl.CostEstimate(
            flops=HEADS * 4 * PATCHES * PATCHES * LANES,
            bytes_accessed=8 * PATCHES * WIDE,
            transcendentals=HEADS * PATCHES * PATCHES,
        ),
        name="attend",
    )(qkv, qkv, qkv, gcol, grow)


def attend_back(qkv, gcol, grow, grads):
    block = pl.BlockSpec((PATCHES, LANES), lambda h: (0, h))
    return pl.pallas_call(
        attend_back_kernel,
        grid=(HEADS,),
        out_shape=[jax.ShapeDtypeStruct((PATCHES, WIDE), F32)] * 3
        + [
            jax.ShapeDtypeStruct((HEADS, PATCHES, 1), F32),
            jax.ShapeDtypeStruct((HEADS, 1, PATCHES), F32),
        ],
        in_specs=head_specs() + [block],
        out_specs=[block, block, block]
        + [
            pl.BlockSpec((1, PATCHES, 1), lambda h: (h, 0, 0)),
            pl.BlockSpec((1, 1, PATCHES), lambda h: (h, 0, 0)),
        ],
        cost_estimate=pl.CostEstimate(
            flops=HEADS * 10 * PATCHES * PATCHES * LANES,
            bytes_accessed=20 * PATCHES * WIDE,
            transcendentals=HEADS * PATCHES * PATCHES,
        ),
        name="attend_back",
    )(qkv, qkv, qkv, gcol, grow, grads)


def pad_heads(source, axis):
    widths = [(0, 0)] * source.ndim
    widths[axis] = (0, LANES - HD)
    return jnp.pad(source, widths)


def pad_cells(grid):
    return jnp.pad(grid, ((1, 1), (1, 1), (0, 0)))


def pick(source, axis, index):
    return lax.dynamic_index_in_dim(source, index, axis, keepdims=False)


MESH = pl.DeviceIdType.MESH


def greet(peers):
    barrier = pltpu.get_barrier_semaphore()
    for peer in peers:
        pl.semaphore_signal(barrier, inc=1, device_id=peer, device_id_type=MESH)
    pl.semaphore_wait(barrier, len(peers))


def team_peers():
    place = lax.axis_index("pos")
    up, side, core = place // 4, (place // 2) % 2, place % 2
    return up, side, core


def seat(up, side, core):
    return up * 4 + side * 2 + core


def team_gather_kernel(x_ref, out_ref, send_sem, recv_sem):
    up, side, core = team_peers()
    mine = seat(up, side, core)
    above, beside, across = (
        seat(1 - up, side, core),
        seat(up, 1 - side, core),
        seat(1 - up, 1 - side, core),
    )
    twin = {"pos": seat(up, side, 1 - core)}
    to_up = {"pos": above}
    to_side = {"pos": beside}
    greet((to_up, to_side, twin))
    rows = x_ref.shape[0]
    parts = (pl.ds(0, rows // 2), pl.ds(rows // 2, rows // 2))

    def send(slot, source, owner, part, peer):
        copy = pltpu.make_async_remote_copy(
            src_ref=source,
            dst_ref=out_ref.at[owner, part],
            send_sem=send_sem.at[slot],
            recv_sem=recv_sem.at[slot],
            device_id=peer,
            device_id_type=MESH,
        )
        copy.start()
        return copy

    held = [
        send(0, x_ref.at[parts[0]], mine, parts[0], to_up),
        send(1, x_ref.at[parts[1]], mine, parts[1], to_side),
        send(2, x_ref.at[parts[1]], mine, parts[1], to_up),
        send(3, x_ref.at[parts[0]], mine, parts[0], to_side),
        send(4, x_ref.at[parts[0]], mine, parts[0], twin),
        send(5, x_ref.at[parts[1]], mine, parts[1], twin),
    ]
    out_ref[mine] = x_ref[...]
    held[0].wait_recv()
    held.append(send(6, out_ref.at[above, parts[0]], above, parts[0], to_side))
    held.append(send(7, out_ref.at[above, parts[0]], above, parts[0], twin))
    held[1].wait_recv()
    held.append(send(8, out_ref.at[beside, parts[1]], beside, parts[1], to_up))
    held.append(send(9, out_ref.at[beside, parts[1]], beside, parts[1], twin))
    held[2].wait_recv()
    held.append(send(10, out_ref.at[above, parts[1]], above, parts[1], twin))
    held[3].wait_recv()
    held.append(send(11, out_ref.at[beside, parts[0]], beside, parts[0], twin))
    held[6].wait_recv()
    held.append(send(12, out_ref.at[across, parts[0]], across, parts[0], twin))
    held[8].wait_recv()
    held.append(send(13, out_ref.at[across, parts[1]], across, parts[1], twin))
    for slot in (4, 5, 7, 9, 10, 11, 12, 13):
        held[slot].wait_recv()
    for copy in held:
        copy.wait_send()


def team_gather(source):
    rows, width = source.shape
    vmem = pl.BlockSpec(memory_space=pltpu.VMEM)
    return pl.pallas_call(
        team_gather_kernel,
        out_shape=jax.ShapeDtypeStruct((TEAM, rows, width), source.dtype),
        in_specs=[vmem],
        out_specs=vmem,
        scratch_shapes=[pltpu.SemaphoreType.DMA((14,)), pltpu.SemaphoreType.DMA((14,))],
        compiler_params=pltpu.CompilerParams(collective_id=1, has_side_effects=True),
        name="team_gather",
    )(source).reshape(TEAM * rows, width)


def team_scatter_kernel(x_ref, out_ref, twins, low, first, turned, second, send_sem, recv_sem):
    up, side, core = team_peers()
    twin = {"pos": seat(up, side, 1 - core)}
    to_up = {"pos": seat(1 - up, side, core)}
    to_side = {"pos": seat(up, 1 - side, core)}
    greet((to_up, to_side, twin))
    rows = x_ref.shape[1]
    part_rows = rows // 2
    parts = (pl.ds(0, part_rows), pl.ds(part_rows, part_rows))

    def send(slot, source, target, peer):
        copy = pltpu.make_async_remote_copy(
            src_ref=source,
            dst_ref=target,
            send_sem=send_sem.at[slot],
            recv_sem=recv_sem.at[slot],
            device_id=peer,
            device_id_type=MESH,
        )
        copy.start()
        return copy

    chips = ((1 - up, 1 - side), (1 - up, side), (up, 1 - side), (up, side))
    held = []
    for slot, (u, s) in enumerate(chips):
        held.append(send(slot, x_ref.at[seat(u, s, 1 - core)], twins.at[u * 2 + s], twin))

    def merge(slot):
        u, s = chips[slot]
        held[slot].wait_recv()
        low[u * 2 + s] = (
            x_ref[seat(u, s, core)].astype(F32) + twins[u * 2 + s].astype(F32)
        ).astype(BF16)

    merge(0)
    a_far = send(4, low.at[(1 - up) * 2 + 1 - side, parts[0]], first.at[1 - side], to_up)
    b_far = send(5, low.at[(1 - up) * 2 + 1 - side, parts[1]], first.at[2 + 1 - up], to_side)
    merge(1)
    a_near = send(6, low.at[(1 - up) * 2 + side, parts[0]], first.at[side], to_up)
    merge(2)
    b_near = send(7, low.at[up * 2 + 1 - side, parts[1]], first.at[2 + up], to_side)
    merge(3)
    a_far.wait_recv()
    turned[0] = (
        low[up * 2 + 1 - side, parts[0]].astype(F32) + first[1 - side].astype(F32)
    ).astype(BF16)
    a_last = send(8, turned.at[0], second.at[0], to_side)
    b_far.wait_recv()
    turned[1] = (
        low[(1 - up) * 2 + side, parts[1]].astype(F32) + first[2 + 1 - up].astype(F32)
    ).astype(BF16)
    b_last = send(9, turned.at[1], second.at[1], to_up)
    a_near.wait_recv()
    b_near.wait_recv()
    a_last.wait_recv()
    out_ref[parts[0]] = (
        low[up * 2 + side, parts[0]].astype(F32)
        + first[side].astype(F32)
        + second[0].astype(F32)
    )
    b_last.wait_recv()
    out_ref[parts[1]] = (
        low[up * 2 + side, parts[1]].astype(F32)
        + first[2 + up].astype(F32)
        + second[1].astype(F32)
    )
    for copy in held + [a_far, b_far, a_near, b_near, a_last, b_last]:
        copy.wait_send()


def team_scatter(partial):
    rows, width = partial.shape[0] // TEAM, partial.shape[1]
    vmem = pl.BlockSpec(memory_space=pltpu.VMEM)
    return pl.pallas_call(
        team_scatter_kernel,
        out_shape=jax.ShapeDtypeStruct((rows, width), F32),
        in_specs=[vmem],
        out_specs=vmem,
        scratch_shapes=[
            pltpu.VMEM((4, rows, width), BF16),
            pltpu.VMEM((4, rows, width), BF16),
            pltpu.VMEM((4, rows // 2, width), BF16),
            pltpu.VMEM((2, rows // 2, width), BF16),
            pltpu.VMEM((2, rows // 2, width), BF16),
            pltpu.SemaphoreType.DMA((10,)),
            pltpu.SemaphoreType.DMA((10,)),
        ],
        compiler_params=pltpu.CompilerParams(collective_id=2, has_side_effects=True),
        name="team_scatter",
    )(partial.astype(BF16).reshape(TEAM, rows, width))


def flat_peer(index, sizes):
    halves, groups = sizes
    where = {"grp": (index // TEAM) % groups, "pos": index % TEAM}
    if halves > 1:
        where["items"] = index // (TEAM * groups)
    return where


def flat_index(sizes):
    halves, groups = sizes
    here = lax.axis_index("grp") * TEAM + lax.axis_index("pos")
    if halves > 1:
        here = here + lax.axis_index("items") * (TEAM * groups)
    return here


def greet_all(me, total, sizes):
    barrier = pltpu.get_barrier_semaphore()

    def call(step, carry):
        pl.semaphore_signal(
            barrier,
            inc=1,
            device_id=flat_peer((me + step) % total, sizes),
            device_id_type=MESH,
        )
        return carry

    lax.fori_loop(1, total, call, 0)
    pl.semaphore_wait(barrier, total - 1)


def send_all(me, total, sizes, source_of, target, send_sem, recv_sem, whole):
    def describe(step):
        peer = (me + step) % total
        return pltpu.make_async_remote_copy(
            src_ref=source_of(peer),
            dst_ref=target,
            send_sem=send_sem,
            recv_sem=recv_sem,
            device_id=flat_peer(peer, sizes),
            device_id_type=MESH,
        )

    def start(step, carry):
        describe(step).start()
        return carry

    lax.fori_loop(1, total, start, 0)
    everything = pltpu.make_async_remote_copy(
        src_ref=whole.at[pl.ds(0, total - 1)],
        dst_ref=whole.at[pl.ds(0, total - 1)],
        send_sem=send_sem,
        recv_sem=recv_sem,
        device_id=flat_peer((me + 1) % total, sizes),
        device_id_type=MESH,
    )
    everything.wait_recv()
    everything.wait_send()


def small_gather_kernel(sizes, x_ref, out_ref, send_sem, recv_sem):
    total = sizes[0] * sizes[1] * TEAM
    me = flat_index(sizes)
    greet_all(me, total, sizes)
    out_ref[me] = x_ref[...]
    send_all(me, total, sizes, lambda peer: x_ref, out_ref.at[me], send_sem, recv_sem, out_ref)


def small_gather(source, sizes, number):
    total = sizes[0] * sizes[1] * TEAM
    count = source.shape[0]
    lines = -(-count // 1024) * 8
    padded = jnp.pad(source, (0, lines * 128 - count)).reshape(lines, 128)
    vmem = pl.BlockSpec(memory_space=pltpu.VMEM)
    out = pl.pallas_call(
        functools.partial(small_gather_kernel, sizes),
        out_shape=jax.ShapeDtypeStruct((total, lines, 128), F32),
        in_specs=[vmem],
        out_specs=vmem,
        scratch_shapes=[pltpu.SemaphoreType.DMA, pltpu.SemaphoreType.DMA],
        compiler_params=pltpu.CompilerParams(collective_id=number, has_side_effects=True),
        name="small_gather",
    )(padded)
    return out.reshape(total, lines * 128)[:, :count]


def small_scatter_kernel(sizes, x_ref, out_ref, came, send_sem, recv_sem):
    halves, groups = sizes
    total = halves * groups * TEAM
    line = groups * TEAM
    me = flat_index(sizes)
    greet_all(me, total, sizes)
    came[me] = x_ref[me % line]
    send_all(
        me, total, sizes, lambda peer: x_ref.at[peer % line], came.at[me], send_sem, recv_sem, came
    )

    def item(number, carry):
        out_ref[number] = jnp.sum(came[pl.ds(number * TEAM, TEAM)], axis=0)
        return carry

    lax.fori_loop(0, halves * groups, item, 0)


def small_scatter(source, sizes, number):
    halves, groups = sizes
    line, count = source.shape
    lines = -(-count // 1024) * 8
    padded = jnp.pad(source, ((0, 0), (0, lines * 128 - count))).reshape(line, lines, 128)
    vmem = pl.BlockSpec(memory_space=pltpu.VMEM)
    out = pl.pallas_call(
        functools.partial(small_scatter_kernel, sizes),
        out_shape=jax.ShapeDtypeStruct((halves * groups, lines, 128), F32),
        in_specs=[vmem],
        out_specs=vmem,
        scratch_shapes=[
            pltpu.VMEM((halves * line, lines, 128), F32),
            pltpu.SemaphoreType.DMA,
            pltpu.SemaphoreType.DMA,
        ],
        compiler_params=pltpu.CompilerParams(collective_id=number, has_side_effects=True),
        name="small_scatter",
    )(padded)
    return out.reshape(halves * groups, lines * 128)[:, :count]


def small_sum_kernel(sizes, x_ref, out_ref, came, summed, sems):
    total = sizes[0] * sizes[1] * TEAM
    me = flat_index(sizes)
    greet_all(me, total, sizes)
    came[me] = x_ref[me]
    send_all(
        me, total, sizes, lambda peer: x_ref.at[peer], came.at[me], sems.at[0], sems.at[1], came
    )
    result = jnp.sum(came[...], axis=0)
    summed[...] = result
    out_ref[me] = result
    send_all(
        me, total, sizes, lambda peer: summed, out_ref.at[me], sems.at[2], sems.at[3], out_ref
    )


def small_sum(source, sizes, number):
    total = sizes[0] * sizes[1] * TEAM
    count = source.shape[0]
    lines = -(-count // (1024 * total)) * 8
    padded = jnp.pad(source, (0, total * lines * 128 - count)).reshape(total, lines, 128)
    vmem = pl.BlockSpec(memory_space=pltpu.VMEM)
    out = pl.pallas_call(
        functools.partial(small_sum_kernel, sizes),
        out_shape=jax.ShapeDtypeStruct((total, lines, 128), F32),
        in_specs=[vmem],
        out_specs=vmem,
        scratch_shapes=[
            pltpu.VMEM((total, lines, 128), F32),
            pltpu.VMEM((lines, 128), F32),
            pltpu.SemaphoreType.DMA((4,)),
        ],
        compiler_params=pltpu.CompilerParams(collective_id=number, has_side_effects=True),
        name="small_sum",
    )(padded)
    return out.reshape(-1)[:count]


def on_device(
    groups,
    patches,
    condition,
    lengths,
    modulator,
    baseline,
    projector,
    forgetter,
    retention,
    smoother,
    pedestal,
    combiner,
    displacement,
    expander,
    thresholds,
    reducer,
    leveling,
    cotangent,
):
    rows_axes = ("grp", "pos")
    half = lax.axis_index("items")
    halves = lax.axis_size("items")
    group = lax.axis_index("grp")
    place = lax.axis_index("pos")
    devices = groups * TEAM
    depth = D // devices
    inner = FF // devices
    columns = 6 * D // devices
    whole_heads = depth == HD
    upstream = cotangent.astype(F32).reshape(TOK_DEV, D)
    inputs = patches.astype(F32).reshape(TOK_DEV, D)

    condition_float = condition.astype(F32)
    squashed = jax.nn.silu(condition_float).astype(BF16)
    squashed_other = lax.ppermute(squashed, "items", [(0, 1), (1, 0)])
    squashed_every = jnp.concatenate(
        [
            jnp.where(half == 0, squashed, squashed_other),
            jnp.where(half == 0, squashed_other, squashed),
        ],
        axis=0,
    )
    modulation_piece = (dot(squashed, modulator) + baseline).astype(BF16).T
    def group_gather(source):
        if groups != 2:
            return lax.all_gather(source, "grp", axis=0, tiled=True)
        other = lax.ppermute(source, "grp", [(0, 1), (1, 0)])
        first = group == 0
        return jnp.concatenate(
            [jnp.where(first, source, other), jnp.where(first, other, source)], axis=0
        )

    project_cut = jnp.concatenate(
        [
            projector.reshape(depth, 3, HEADS, TEAM, HD)
            .transpose(3, 0, 1, 2, 4)
            .reshape(TEAM, depth, 3 * HEADS * HD),
            forgetter.reshape(depth, HEADS, TEAM).transpose(2, 0, 1),
        ],
        axis=2,
    )
    project_part = lax.all_to_all(project_cut, "pos", split_axis=0, concat_axis=0, tiled=True)
    project_part, modulation_piece, expander, reducer, combiner = lax.optimization_barrier(
        (project_part, modulation_piece, expander, reducer, combiner)
    )
    project_mine = group_gather(project_part).reshape(D, -1)
    modulation_all = small_gather(
        modulation_piece.T.astype(F32).reshape(-1), (1, groups), 3
    ).reshape(devices, groups, columns)
    modulation = pick(modulation_all, 1, group).reshape(-1)
    shift_one, scale_one, gate_one, shift_two, scale_two, gate_two = [
        modulation[part * D : (part + 1) * D] for part in range(6)
    ]

    project_wide = jnp.concatenate(
        [
            pad_heads(project_mine[:, : 3 * HEADS * HD].reshape(D, 3 * HEADS, HD), 2).reshape(
                D, 3 * WIDE
            ),
            jnp.pad(project_mine[:, 3 * HEADS * HD :], ((0, 0), (0, LANES - HEADS))),
        ],
        axis=1,
    )
    expand_cut = (
        expander.reshape(depth, groups, TEAM, inner)
        .transpose(2, 0, 1, 3)
        .reshape(TEAM, depth, groups * inner)
    )
    expand_part = lax.all_to_all(expand_cut, "pos", split_axis=0, concat_axis=0, tiled=True)
    expand_mine = group_gather(expand_part).reshape(D, groups * inner)
    reduce_mine = group_gather(reducer)
    if whole_heads:
        combine_mine = group_gather(combiner).reshape(HEADS, HD, D)
    else:
        combine_all = lax.all_gather(combiner, rows_axes, axis=0, tiled=True)
        combine_mine = pick(combine_all.reshape(HEADS, TEAM, HD, D), 1, place)
    combine_wide = pad_heads(combine_mine, 1).reshape(WIDE, D)
    thresholds_mine = pick(thresholds.reshape(groups, TEAM, inner), 1, place).reshape(-1)
    retention_mine = pick(retention.reshape(HEADS, TEAM), 1, place)
    kernel = pad_heads(pick(smoother.reshape(9, HEADS, TEAM, HD), 2, place), 2).reshape(9, WIDE)
    offset = pad_heads(pick(pedestal.reshape(HEADS, TEAM, HD), 1, place), 1).reshape(WIDE)

    hidden = modulate(inputs, shift_one, scale_one).astype(BF16)
    hidden_all = team_gather(hidden)
    projected = dot(hidden_all, project_wide)
    forget_logit = projected[:, 3 * WIDE : 3 * WIDE + HEADS] + retention_mine
    decays = (jax.nn.log_sigmoid(forget_logit) / 16.0).astype(BF16)
    index = jnp.arange(PATCHES, dtype=jnp.int32)
    length = pick(lengths, 0, group)
    validity = (index < length)[:, None]
    is_query = jnp.arange(3 * WIDE) < WIDE
    keep = validity | is_query[None, :]
    qkv = jnp.where(keep, projected[:, : 3 * WIDE], 0.0).astype(BF16)
    order = column_place(index)
    causal = (order[None, :] <= order[:, None]).astype(BF16)
    summed = dot(causal, decays)
    gcol = summed.T[:, :, None]
    grow = summed.T[:, None, :]
    attended = attend(qkv, gcol, grow)

    attended_grid = attended.astype(F32).reshape(GRID, GRID, WIDE)
    attended_padded = pad_cells(attended_grid)
    smoothed = jnp.zeros_like(attended_grid) + offset
    for tap in range(9):
        down, right = tap // 3, tap % 3
        smoothed = (
            smoothed + kernel[tap] * attended_padded[down : down + GRID, right : right + GRID]
        )
    smoothed = smoothed.astype(BF16).reshape(PATCHES, WIDE)
    branch = team_scatter(dot(smoothed, combine_wide)) + displacement
    middle = inputs + gate_one * branch
    hidden_two = modulate(middle, shift_two, scale_two).astype(BF16)
    hidden_two_all = team_gather(hidden_two)
    expanded = dot(hidden_two_all, expand_mine) + thresholds_mine
    activated = jax.nn.gelu(expanded, approximate=True).astype(BF16)
    reduced = team_scatter(dot(activated, reduce_mine)) + leveling
    block_output = (middle + gate_two * reduced).astype(BF16).reshape(ROWS_DEV, GRID, D)

    def swap_add(share):
        low = share.astype(BF16)
        other = lax.ppermute(low, "items", [(0, 1), (1, 0)])
        return low.astype(F32) + other.astype(F32)

    def to_owners(source):
        pieces = source.reshape(devices, depth, source.shape[1])
        arrived = lax.all_to_all(pieces, rows_axes, split_axis=0, concat_axis=0, tiled=True)
        arrived = arrived.reshape(groups, TEAM, depth, source.shape[1])
        return jnp.sum(arrived.astype(F32), axis=0).astype(BF16)

    def group_scatter(source):
        low = source.astype(BF16)
        if groups != 2:
            arrived = lax.all_to_all(low, "grp", split_axis=0, concat_axis=0, tiled=True)
            return jnp.sum(arrived.astype(F32), axis=0)
        arrived = lax.ppermute(pick(low, 0, 1 - group), "grp", [(0, 1), (1, 0)])
        return pick(low, 0, group).astype(F32) + arrived.astype(F32)

    gate_two_grad = jnp.sum(upstream * reduced, axis=0)
    reduced_grad = (gate_two * upstream).astype(BF16)
    leveling_grad = jnp.sum(reduced_grad.astype(F32), axis=0)
    reduced_grad_all = team_gather(reduced_grad)
    reducer_grad = outer_sum(activated, reduced_grad_all)
    reducer_out = swap_add(group_scatter(reducer_grad.reshape(groups, inner, D)))
    activated_grad = back_dot(reduced_grad_all, reduce_mine)
    pull = jax.vjp(lambda v: jax.nn.gelu(v, approximate=True), expanded)[1]
    expanded_grad = pull(activated_grad)[0].astype(BF16)
    thresholds_grad = jnp.sum(expanded_grad.astype(F32), axis=0)
    expander_grad = outer_sum(hidden_two_all, expanded_grad)
    expander_out = swap_add(
        to_owners(expander_grad.astype(BF16))
        .reshape(TEAM, depth, groups, inner)
        .transpose(1, 2, 0, 3)
        .reshape(depth, FF)
    )
    hidden_two_grad = team_scatter(back_dot(expanded_grad, expand_mine))
    second_pull = jax.vjp(modulate, middle, shift_two, scale_two)[1]
    middle_part, shift_two_grad, scale_two_grad = second_pull(hidden_two_grad)
    middle_grad = upstream + middle_part
    gate_one_grad = jnp.sum(middle_grad * branch, axis=0)
    branch_grad = (gate_one * middle_grad).astype(BF16)
    displacement_grad = jnp.sum(branch_grad.astype(F32), axis=0)
    branch_grad_all = team_gather(branch_grad)
    combiner_grad = outer_sum(smoothed, branch_grad_all)
    combiner_low = combiner_grad.reshape(HEADS, LANES, D)[:, :HD]
    if whole_heads:
        combiner_share = group_scatter(combiner_low)
    else:
        placed = jnp.where(
            (jnp.arange(TEAM) == place)[None, :, None, None], combiner_low[:, None], 0.0
        )
        combiner_share = lax.psum_scatter(
            placed.reshape(D, D), rows_axes, scatter_dimension=0, tiled=True
        )
    combiner_out = swap_add(combiner_share)
    smoothed_grad = back_dot(branch_grad_all, combine_wide).astype(BF16).astype(F32)
    pedestal_grad = jnp.sum(smoothed_grad, axis=0)
    grad_grid = smoothed_grad.reshape(GRID, GRID, WIDE)
    grad_padded = pad_cells(grad_grid)
    tap_grads = []
    attended_grad = jnp.zeros_like(grad_grid)
    for tap in range(9):
        down, right = tap // 3, tap % 3
        tap_grads.append(
            jnp.sum(
                grad_grid * attended_padded[down : down + GRID, right : right + GRID], axis=(0, 1)
            )
        )
        attended_grad = (
            attended_grad
            + kernel[tap] * grad_padded[2 - down : 2 - down + GRID, 2 - right : 2 - right + GRID]
        )
    tap_stack = jnp.stack(tap_grads)
    attended_grad = attended_grad.astype(BF16).reshape(PATCHES, WIDE)
    dq, dk, dv, row_sum, col_sum = attend_back(qkv, gcol, grow, attended_grad)
    moment = row_sum[:, :, 0] - col_sum[:, 0, :]
    decay_grad = lax.dot_general(
        causal.astype(F32),
        moment,
        (((0,), (1,)), ((), ())),
        precision=HIGH,
        preferred_element_type=F32,
    )
    forget_grad = (decay_grad * jax.nn.sigmoid(-forget_logit) / 16.0).astype(BF16)
    retention_grad = jnp.sum(forget_grad.astype(F32), axis=0)
    project_grad = jnp.concatenate(
        [
            dq.astype(BF16),
            jnp.where(validity, dk, 0.0).astype(BF16),
            jnp.where(validity, dv, 0.0).astype(BF16),
            jnp.pad(forget_grad, ((0, 0), (0, LANES - HEADS))),
        ],
        axis=1,
    )
    projector_grad = outer_sum(hidden_all, project_grad)
    hidden_grad = team_scatter(back_dot(project_grad, project_wide))
    first_pull = jax.vjp(modulate, inputs, shift_one, scale_one)[1]
    inputs_part, shift_one_grad, scale_one_grad = first_pull(hidden_grad)
    patches_grad = (middle_grad + inputs_part).astype(BF16).reshape(ROWS_DEV, GRID, D)

    projector_low = projector_grad.astype(BF16)
    project_share = to_owners(
        jnp.concatenate(
            [
                projector_low[:, : 3 * WIDE].reshape(D, 3 * HEADS, LANES)[:, :, :HD].reshape(
                    D, 3 * HEADS * HD
                ),
                projector_low[:, 3 * WIDE : 3 * WIDE + HEADS],
            ],
            axis=1,
        )
    )
    projector_out = swap_add(
        project_share[:, :, : 3 * HEADS * HD]
        .reshape(TEAM, depth, 3, HEADS, HD)
        .transpose(1, 2, 3, 0, 4)
        .reshape(depth, 3 * D)
    )
    forgetter_out = swap_add(
        project_share[:, :, 3 * HEADS * HD :].transpose(1, 2, 0).reshape(depth, H)
    )

    modulation_grad = jnp.concatenate(
        [
            shift_one_grad,
            scale_one_grad,
            gate_one_grad,
            shift_two_grad,
            scale_two_grad,
            gate_two_grad,
        ]
    ).reshape(devices, columns)
    rows_every = small_scatter(modulation_grad, (halves, groups), 4)
    modulator_out = lax.dot_general(
        squashed_every.astype(F32), rows_every, (((0,), (0,)), ((), ())), precision=HIGH
    )
    baseline_out = jnp.sum(rows_every, axis=0)
    modulation_rows = pick(rows_every.reshape(halves, groups, columns), 0, half)
    squashed_grad = jnp.dot(modulation_rows, modulator.astype(F32).T, precision=HIGH)

    def spot(value, shape, axis, at):
        where = (jnp.arange(shape[axis]) == at).reshape(
            [-1 if spot_axis == axis else 1 for spot_axis in range(len(shape))]
        )
        return jnp.where(where, jnp.expand_dims(value, axis), 0.0).reshape(-1)

    parts = [
        spot(squashed_grad, (halves, groups, D), 0, half),
        spot(retention_grad, (HEADS, TEAM), 1, place),
        spot(tap_stack.reshape(9, HEADS, LANES)[:, :, :HD], (9, HEADS, TEAM, HD), 2, place),
        spot(pedestal_grad.reshape(HEADS, LANES)[:, :HD], (HEADS, TEAM, HD), 1, place),
        displacement_grad,
        spot(thresholds_grad.reshape(groups, inner), (groups, TEAM, inner), 1, place),
        leveling_grad,
    ]
    total = small_sum(jnp.concatenate(parts), (halves, groups), 5)
    split = []
    start = 0
    for part in parts:
        split.append(total[start : start + part.shape[0]])
        start += part.shape[0]
    squashed_sum = pick(split[0].reshape(halves, groups, D), 0, half)
    silu_pull = jax.vjp(jax.nn.silu, condition_float)[1]
    condition_grad = silu_pull(squashed_sum)[0]
    return (
        block_output,
        patches_grad,
        condition_grad,
        modulator_out,
        baseline_out,
        projector_out,
        forgetter_out,
        split[1],
        split[2].reshape(9, D),
        split[3],
        combiner_out,
        split[4],
        expander_out,
        split[5],
        reducer_out,
        split[6],
    )


def solution(mesh):
    rows = mesh.shape["rows"]
    groups = rows // TEAM
    fine = Mesh(
        mesh.devices.reshape(mesh.shape["items"], groups, TEAM), ("items", "grp", "pos")
    )
    line = ("grp", "pos")
    tokens = P(("items", "grp", "pos"), None, None)
    in_specs = (
        tokens,
        P("items", None),
        P("items"),
        P(None, line),
        P(line),
        P(line, None),
        P(line, None),
        P(),
        P(),
        P(),
        P(line, None),
        P(),
        P(line, None),
        P(),
        P(line, None),
        P(),
        tokens,
    )
    out_specs = (
        tokens,
        tokens,
        P("items", None),
        P(None, line),
        P(line),
        P(line, None),
        P(line, None),
        P(),
        P(),
        P(),
        P(line, None),
        P(),
        P(line, None),
        P(),
        P(line, None),
        P(),
    )
    return jax.shard_map(
        functools.partial(on_device, groups),
        mesh=fine,
        in_specs=in_specs,
        out_specs=out_specs,
        check_vma=False,
    )
```

```python
import functools

import jax
import jax.numpy as jnp
from jax import lax
from jax.experimental import pallas as pl
from jax.experimental.pallas import tpu as pltpu
from jax.sharding import Mesh, PartitionSpec as P

H = 16
HD = 72
D = 1152
FF = 4608
GRID = 32
PATCHES = 1024
ROWS_DEV = 4
TOK_DEV = 128
TEAM = GRID // ROWS_DEV
HEADS = H // TEAM
LANES = 128
WIDE = HEADS * LANES
STRIP = 256

EPS = 1e-06
HIGH = lax.Precision.HIGHEST
F32 = jnp.float32
BF16 = jnp.bfloat16
FACTOR = HD ** (-0.5)


def modulate(values, offset, stretch):
    centred = values - jnp.mean(values, axis=-1, keepdims=True)
    spread = jnp.mean(centred * centred, axis=-1, keepdims=True)
    return centred * lax.rsqrt(spread + EPS) * (1.0 + stretch) + offset


def dot(left, right):
    return jnp.dot(left, right, preferred_element_type=F32)


def outer_sum(left, right):
    return lax.dot_general(left, right, (((0,), (0,)), ((), ())), preferred_element_type=F32)


def back_dot(gradient, matrix):
    return lax.dot_general(gradient, matrix, (((1,), (1,)), ((), ())), preferred_element_type=F32)


def column_place(index):
    return (index & (GRID - 1)) * GRID + (index >> 5)


def strip_weights(start, gcol, grow):
    rows = lax.broadcasted_iota(jnp.int32, (STRIP, PATCHES), 0) + start
    cols = lax.broadcasted_iota(jnp.int32, (STRIP, PATCHES), 1)
    causal = column_place(cols) <= column_place(rows)
    return jnp.exp(jnp.where(causal, gcol - grow, -1e30))


def attend_kernel(q_ref, k_ref, v_ref, gcol_ref, grow_ref, out_ref):
    keys = k_ref[...]
    values = v_ref[...]
    grow = grow_ref[0]

    def strip(number, carry):
        start = pl.multiple_of(number * STRIP, STRIP)
        here = pl.ds(start, STRIP)
        weights = strip_weights(start, gcol_ref[0, here, :], grow)
        scores = back_dot(q_ref[here, :], keys) * weights
        out_ref[here, :] = (dot(scores.astype(BF16), values) * FACTOR).astype(BF16)
        return carry

    lax.fori_loop(0, PATCHES // STRIP, strip, 0)


def attend_back_kernel(
    q_ref, k_ref, v_ref, gcol_ref, grow_ref, do_ref, dq_ref, dk_ref, dv_ref, row_ref, col_ref
):
    keys = k_ref[...]
    values = v_ref[...]
    grow = grow_ref[0]
    dk_ref[...] = jnp.zeros_like(dk_ref)
    dv_ref[...] = jnp.zeros_like(dv_ref)
    col_ref[...] = jnp.zeros_like(col_ref)

    def strip(number, carry):
        start = pl.multiple_of(number * STRIP, STRIP)
        here = pl.ds(start, STRIP)
        queries = q_ref[here, :]
        grads = do_ref[here, :]
        weights = strip_weights(start, gcol_ref[0, here, :], grow)
        scores = back_dot(queries, keys) * weights
        back = back_dot(grads, values)
        pulled = (back * weights).astype(BF16)
        moment = back * scores
        dv_ref[...] += outer_sum(scores.astype(BF16), grads)
        dk_ref[...] += outer_sum(pulled, queries)
        dq_ref[here, :] = dot(pulled, keys) * FACTOR
        row_ref[0, here, :] = jnp.sum(moment, axis=1, keepdims=True) * FACTOR
        col_ref[0] += jnp.sum(moment, axis=0, keepdims=True) * FACTOR
        return carry

    lax.fori_loop(0, PATCHES // STRIP, strip, 0)
    dk_ref[...] *= FACTOR
    dv_ref[...] *= FACTOR


def head_specs():
    return [
        pl.BlockSpec((PATCHES, LANES), lambda h: (0, h)),
        pl.BlockSpec((PATCHES, LANES), lambda h: (0, HEADS + h)),
        pl.BlockSpec((PATCHES, LANES), lambda h: (0, 2 * HEADS + h)),
        pl.BlockSpec((1, PATCHES, 1), lambda h: (h, 0, 0)),
        pl.BlockSpec((1, 1, PATCHES), lambda h: (h, 0, 0)),
    ]


def attend(qkv, gcol, grow):
    return pl.pallas_call(
        attend_kernel,
        grid=(HEADS,),
        out_shape=jax.ShapeDtypeStruct((PATCHES, WIDE), BF16),
        in_specs=head_specs(),
        out_specs=pl.BlockSpec((PATCHES, LANES), lambda h: (0, h)),
        cost_estimate=pl.CostEstimate(
            flops=HEADS * 4 * PATCHES * PATCHES * LANES,
            bytes_accessed=8 * PATCHES * WIDE,
            transcendentals=HEADS * PATCHES * PATCHES,
        ),
        name="attend",
    )(qkv, qkv, qkv, gcol, grow)


def attend_back(qkv, gcol, grow, grads):
    block = pl.BlockSpec((PATCHES, LANES), lambda h: (0, h))
    return pl.pallas_call(
        attend_back_kernel,
        grid=(HEADS,),
        out_shape=[jax.ShapeDtypeStruct((PATCHES, WIDE), F32)] * 3
        + [
            jax.ShapeDtypeStruct((HEADS, PATCHES, 1), F32),
            jax.ShapeDtypeStruct((HEADS, 1, PATCHES), F32),
        ],
        in_specs=head_specs() + [block],
        out_specs=[block, block, block]
        + [
            pl.BlockSpec((1, PATCHES, 1), lambda h: (h, 0, 0)),
            pl.BlockSpec((1, 1, PATCHES), lambda h: (h, 0, 0)),
        ],
        cost_estimate=pl.CostEstimate(
            flops=HEADS * 10 * PATCHES * PATCHES * LANES,
            bytes_accessed=20 * PATCHES * WIDE,
            transcendentals=HEADS * PATCHES * PATCHES,
        ),
        name="attend_back",
    )(qkv, qkv, qkv, gcol, grow, grads)


def pad_heads(source, axis):
    widths = [(0, 0)] * source.ndim
    widths[axis] = (0, LANES - HD)
    return jnp.pad(source, widths)


def pad_cells(grid):
    return jnp.pad(grid, ((1, 1), (1, 1), (0, 0)))


def pick(source, axis, index):
    return lax.dynamic_index_in_dim(source, index, axis, keepdims=False)


MESH = pl.DeviceIdType.MESH


def greet(peers):
    barrier = pltpu.get_barrier_semaphore()
    for peer in peers:
        pl.semaphore_signal(barrier, inc=1, device_id=peer, device_id_type=MESH)
    pl.semaphore_wait(barrier, len(peers))


def team_peers():
    place = lax.axis_index("pos")
    up, side, core = place // 4, (place // 2) % 2, place % 2
    return up, side, core


def seat(up, side, core):
    return up * 4 + side * 2 + core


def team_gather_kernel(count, *refs):
    inputs, outputs = refs[:count], refs[count : 2 * count]
    send_sem, recv_sem = refs[2 * count :]
    up, side, core = team_peers()
    mine = seat(up, side, core)
    above, beside, across = (
        seat(1 - up, side, core),
        seat(up, 1 - side, core),
        seat(1 - up, 1 - side, core),
    )
    twin = {"pos": seat(up, side, 1 - core)}
    to_up = {"pos": above}
    to_side = {"pos": beside}
    greet((to_up, to_side, twin))
    rows = inputs[0].shape[0]
    parts = (pl.ds(0, rows // 2), pl.ds(rows // 2, rows // 2))
    held = {}

    def send(which, slot, owner, part, peer, own=False):
        target = outputs[which].at[owner, part]
        copy = pltpu.make_async_remote_copy(
            src_ref=inputs[which].at[part] if own else target,
            dst_ref=target,
            send_sem=send_sem.at[which, slot],
            recv_sem=recv_sem.at[which, slot],
            device_id=peer,
            device_id_type=MESH,
        )
        copy.start()
        held[which, slot] = copy

    for which in range(count):
        send(which, 0, mine, parts[0], to_up, True)
        send(which, 1, mine, parts[1], to_side, True)
        send(which, 2, mine, parts[1], to_up, True)
        send(which, 3, mine, parts[0], to_side, True)
        send(which, 4, mine, parts[0], twin, True)
        send(which, 5, mine, parts[1], twin, True)
    for which in range(count):
        outputs[which][mine] = inputs[which][...]
    for which in range(count):
        held[which, 0].wait_recv()
        send(which, 6, above, parts[0], to_side)
        send(which, 7, above, parts[0], twin)
        held[which, 1].wait_recv()
        send(which, 8, beside, parts[1], to_up)
        send(which, 9, beside, parts[1], twin)
        held[which, 2].wait_recv()
        send(which, 10, above, parts[1], twin)
        held[which, 3].wait_recv()
        send(which, 11, beside, parts[0], twin)
    for which in range(count):
        held[which, 6].wait_recv()
        send(which, 12, across, parts[0], twin)
        held[which, 8].wait_recv()
        send(which, 13, across, parts[1], twin)
    for which in range(count):
        for slot in (4, 5, 7, 9, 10, 11, 12, 13):
            held[which, slot].wait_recv()
    for copy in held.values():
        copy.wait_send()


def team_gather(*sources):
    rows, width = sources[0].shape
    count = len(sources)
    vmem = pl.BlockSpec(memory_space=pltpu.VMEM)
    outs = pl.pallas_call(
        functools.partial(team_gather_kernel, count),
        out_shape=[jax.ShapeDtypeStruct((TEAM, rows, width), source.dtype) for source in sources],
        in_specs=[vmem] * count,
        out_specs=[vmem] * count,
        scratch_shapes=[pltpu.SemaphoreType.DMA((count, 14)), pltpu.SemaphoreType.DMA((count, 14))],
        compiler_params=pltpu.CompilerParams(
            collective_id=2 * count, has_side_effects=True
        ),
    )(*sources)
    outs = [out.reshape(TEAM * rows, width) for out in outs]
    return outs if count > 1 else outs[0]


def team_scatter_kernel(count, *refs):
    inputs, outputs = refs[:count], refs[count : 2 * count]
    twins, low, first, turned, second, send_sem, recv_sem = refs[2 * count :]
    up, side, core = team_peers()
    twin = {"pos": seat(up, side, 1 - core)}
    to_up = {"pos": seat(1 - up, side, core)}
    to_side = {"pos": seat(up, 1 - side, core)}
    greet((to_up, to_side, twin))
    rows = inputs[0].shape[1]
    part_rows = rows // 2
    parts = (pl.ds(0, part_rows), pl.ds(part_rows, part_rows))
    held = {}

    def send(which, slot, source, target, peer):
        copy = pltpu.make_async_remote_copy(
            src_ref=source,
            dst_ref=target,
            send_sem=send_sem.at[which, slot],
            recv_sem=recv_sem.at[which, slot],
            device_id=peer,
            device_id_type=MESH,
        )
        copy.start()
        held[which, slot] = copy

    chips = ((1 - up, 1 - side), (1 - up, side), (up, 1 - side), (up, side))
    far, above, beside, mine = [u * 2 + s for u, s in chips]
    for which in range(count):
        for slot, (u, s) in enumerate(chips):
            send(
                which,
                slot,
                inputs[which].at[seat(u, s, 1 - core)],
                twins.at[which, u * 2 + s],
                twin,
            )

    def merge(which, slot):
        u, s = chips[slot]
        held[which, slot].wait_recv()
        low[which, u * 2 + s] = (
            inputs[which][seat(u, s, core)].astype(F32) + twins[which, u * 2 + s].astype(F32)
        ).astype(BF16)

    for which in range(count):
        merge(which, 0)
        send(which, 4, low.at[which, far, parts[0]], first.at[which, 1 - side], to_up)
        send(which, 5, low.at[which, far, parts[1]], first.at[which, 2 + 1 - up], to_side)
        merge(which, 1)
        send(which, 6, low.at[which, above, parts[0]], first.at[which, side], to_up)
        merge(which, 2)
        send(which, 7, low.at[which, beside, parts[1]], first.at[which, 2 + up], to_side)
    for which in range(count):
        merge(which, 3)
    for which in range(count):
        held[which, 4].wait_recv()
        turned[which, 0] = (
            low[which, beside, parts[0]].astype(F32) + first[which, 1 - side].astype(F32)
        ).astype(BF16)
        send(which, 8, turned.at[which, 0], second.at[which, 0], to_side)
        held[which, 5].wait_recv()
        turned[which, 1] = (
            low[which, above, parts[1]].astype(F32) + first[which, 2 + 1 - up].astype(F32)
        ).astype(BF16)
        send(which, 9, turned.at[which, 1], second.at[which, 1], to_up)
    for which in range(count):
        held[which, 6].wait_recv()
        held[which, 8].wait_recv()
        outputs[which][parts[0]] = (
            low[which, mine, parts[0]].astype(F32)
            + first[which, side].astype(F32)
            + second[which, 0].astype(F32)
        )
        held[which, 7].wait_recv()
        held[which, 9].wait_recv()
        outputs[which][parts[1]] = (
            low[which, mine, parts[1]].astype(F32)
            + first[which, 2 + up].astype(F32)
            + second[which, 1].astype(F32)
        )
    for copy in held.values():
        copy.wait_send()


def team_scatter(*partials):
    rows, width = partials[0].shape[0] // TEAM, partials[0].shape[1]
    count = len(partials)
    vmem = pl.BlockSpec(memory_space=pltpu.VMEM)
    pieces = [partial.astype(BF16).reshape(TEAM, rows, width) for partial in partials]
    outs = pl.pallas_call(
        functools.partial(team_scatter_kernel, count),
        out_shape=[jax.ShapeDtypeStruct((rows, width), F32)] * count,
        in_specs=[vmem] * count,
        out_specs=[vmem] * count,
        scratch_shapes=[
            pltpu.VMEM((count, 4, rows, width), BF16),
            pltpu.VMEM((count, 4, rows, width), BF16),
            pltpu.VMEM((count, 4, rows // 2, width), BF16),
            pltpu.VMEM((count, 2, rows // 2, width), BF16),
            pltpu.VMEM((count, 2, rows // 2, width), BF16),
            pltpu.SemaphoreType.DMA((count, 10)),
            pltpu.SemaphoreType.DMA((count, 10)),
        ],
        compiler_params=pltpu.CompilerParams(collective_id=2 * count + 1, has_side_effects=True),
    )(*pieces)
    return outs if count > 1 else outs[0]


def flat_peer(index, sizes):
    halves, groups = sizes
    where = {"grp": (index // TEAM) % groups, "pos": index % TEAM}
    if halves > 1:
        where["items"] = index // (TEAM * groups)
    return where


def flat_index(sizes):
    halves, groups = sizes
    here = lax.axis_index("grp") * TEAM + lax.axis_index("pos")
    if halves > 1:
        here = here + lax.axis_index("items") * (TEAM * groups)
    return here


def greet_all(me, total, sizes):
    barrier = pltpu.get_barrier_semaphore()

    def call(step, carry):
        pl.semaphore_signal(
            barrier,
            inc=1,
            device_id=flat_peer((me + step) % total, sizes),
            device_id_type=MESH,
        )
        return carry

    lax.fori_loop(1, total, call, 0)
    pl.semaphore_wait(barrier, total - 1)


def send_all(me, total, sizes, source_of, target, send_sem, recv_sem, whole):
    def describe(step):
        peer = (me + step) % total
        return pltpu.make_async_remote_copy(
            src_ref=source_of(peer),
            dst_ref=target,
            send_sem=send_sem,
            recv_sem=recv_sem,
            device_id=flat_peer(peer, sizes),
            device_id_type=MESH,
        )

    def start(step, carry):
        describe(step).start()
        return carry

    lax.fori_loop(1, total, start, 0)
    everything = pltpu.make_async_remote_copy(
        src_ref=whole.at[pl.ds(0, total - 1)],
        dst_ref=whole.at[pl.ds(0, total - 1)],
        send_sem=send_sem,
        recv_sem=recv_sem,
        device_id=flat_peer((me + 1) % total, sizes),
        device_id_type=MESH,
    )
    everything.wait_recv()
    everything.wait_send()


def small_gather_kernel(sizes, x_ref, out_ref, send_sem, recv_sem):
    total = sizes[0] * sizes[1] * TEAM
    me = flat_index(sizes)
    greet_all(me, total, sizes)
    out_ref[me] = x_ref[...]
    send_all(me, total, sizes, lambda peer: x_ref, out_ref.at[me], send_sem, recv_sem, out_ref)


def small_gather(source, sizes, number):
    total = sizes[0] * sizes[1] * TEAM
    count = source.shape[0]
    lines = -(-count // 1024) * 8
    padded = jnp.pad(source, (0, lines * 128 - count)).reshape(lines, 128)
    vmem = pl.BlockSpec(memory_space=pltpu.VMEM)
    out = pl.pallas_call(
        functools.partial(small_gather_kernel, sizes),
        out_shape=jax.ShapeDtypeStruct((total, lines, 128), F32),
        in_specs=[vmem],
        out_specs=vmem,
        scratch_shapes=[pltpu.SemaphoreType.DMA, pltpu.SemaphoreType.DMA],
        compiler_params=pltpu.CompilerParams(collective_id=number, has_side_effects=True),
        name="small_gather",
    )(padded)
    return out.reshape(total, lines * 128)[:, :count]


def small_scatter_kernel(sizes, x_ref, out_ref, came, send_sem, recv_sem):
    halves, groups = sizes
    total = halves * groups * TEAM
    line = groups * TEAM
    me = flat_index(sizes)
    greet_all(me, total, sizes)
    came[me] = x_ref[me % line]
    send_all(
        me, total, sizes, lambda peer: x_ref.at[peer % line], came.at[me], send_sem, recv_sem, came
    )

    def item(number, carry):
        out_ref[number] = jnp.sum(came[pl.ds(number * TEAM, TEAM)], axis=0)
        return carry

    lax.fori_loop(0, halves * groups, item, 0)


def small_scatter(source, sizes, number):
    halves, groups = sizes
    line, count = source.shape
    lines = -(-count // 1024) * 8
    padded = jnp.pad(source, ((0, 0), (0, lines * 128 - count))).reshape(line, lines, 128)
    vmem = pl.BlockSpec(memory_space=pltpu.VMEM)
    out = pl.pallas_call(
        functools.partial(small_scatter_kernel, sizes),
        out_shape=jax.ShapeDtypeStruct((halves * groups, lines, 128), F32),
        in_specs=[vmem],
        out_specs=vmem,
        scratch_shapes=[
            pltpu.VMEM((halves * line, lines, 128), F32),
            pltpu.SemaphoreType.DMA,
            pltpu.SemaphoreType.DMA,
        ],
        compiler_params=pltpu.CompilerParams(collective_id=number, has_side_effects=True),
        name="small_scatter",
    )(padded)
    return out.reshape(halves * groups, lines * 128)[:, :count]


def small_sum_kernel(sizes, x_ref, out_ref, came, summed, sems):
    total = sizes[0] * sizes[1] * TEAM
    me = flat_index(sizes)
    greet_all(me, total, sizes)
    came[me] = x_ref[me]
    send_all(
        me, total, sizes, lambda peer: x_ref.at[peer], came.at[me], sems.at[0], sems.at[1], came
    )
    result = jnp.sum(came[...], axis=0)
    summed[...] = result
    out_ref[me] = result
    send_all(
        me, total, sizes, lambda peer: summed, out_ref.at[me], sems.at[2], sems.at[3], out_ref
    )


def small_sum(source, sizes, number):
    total = sizes[0] * sizes[1] * TEAM
    count = source.shape[0]
    lines = -(-count // (1024 * total)) * 8
    padded = jnp.pad(source, (0, total * lines * 128 - count)).reshape(total, lines, 128)
    vmem = pl.BlockSpec(memory_space=pltpu.VMEM)
    out = pl.pallas_call(
        functools.partial(small_sum_kernel, sizes),
        out_shape=jax.ShapeDtypeStruct((total, lines, 128), F32),
        in_specs=[vmem],
        out_specs=vmem,
        scratch_shapes=[
            pltpu.VMEM((total, lines, 128), F32),
            pltpu.VMEM((lines, 128), F32),
            pltpu.SemaphoreType.DMA((4,)),
        ],
        compiler_params=pltpu.CompilerParams(collective_id=number, has_side_effects=True),
        name="small_sum",
    )(padded)
    return out.reshape(-1)[:count]


def on_device(groups, *arguments):
    return block(groups, *arguments)


def block(
    groups,
    patches,
    condition,
    lengths,
    modulator,
    baseline,
    projector,
    forgetter,
    retention,
    smoother,
    pedestal,
    combiner,
    displacement,
    expander,
    thresholds,
    reducer,
    leveling,
    cotangent,
):
    rows_axes = ("grp", "pos")
    half = lax.axis_index("items")
    halves = lax.axis_size("items")
    group = lax.axis_index("grp")
    place = lax.axis_index("pos")
    devices = groups * TEAM
    depth = D // devices
    inner = FF // devices
    columns = 6 * D // devices
    whole_heads = depth == HD
    upstream = cotangent.astype(F32).reshape(TOK_DEV, D)
    inputs = patches.astype(F32).reshape(TOK_DEV, D)

    condition_float = condition.astype(F32)
    squashed = jax.nn.silu(condition_float).astype(BF16)
    squashed_other = lax.ppermute(squashed, "items", [(0, 1), (1, 0)])
    squashed_every = jnp.concatenate(
        [
            jnp.where(half == 0, squashed, squashed_other),
            jnp.where(half == 0, squashed_other, squashed),
        ],
        axis=0,
    )
    modulation_piece = (dot(squashed, modulator) + baseline).astype(BF16).T

    def group_gather_in(source):
        if groups != 2:
            return lax.all_gather(source, "grp", axis=0, tiled=True)
        other = lax.ppermute(source, "grp", [(0, 1), (1, 0)])
        first = group == 0
        return jnp.concatenate(
            [jnp.where(first, source, other), jnp.where(first, other, source)], axis=0
        )

    project_cut = jnp.concatenate(
        [
            projector.reshape(depth, 3, HEADS, TEAM, HD)
            .transpose(3, 0, 1, 2, 4)
            .reshape(TEAM, depth, 3 * HEADS * HD),
            forgetter.reshape(depth, HEADS, TEAM).transpose(2, 0, 1),
        ],
        axis=2,
    )
    project_part = lax.all_to_all(project_cut, "pos", split_axis=0, concat_axis=0, tiled=True)
    project_part, modulation_piece, expander, reducer, combiner = lax.optimization_barrier(
        (project_part, modulation_piece, expander, reducer, combiner)
    )
    project_mine = group_gather_in(project_part).reshape(D, -1)
    modulation_all = small_gather(
        modulation_piece.T.astype(F32).reshape(-1), (1, groups), 7
    ).reshape(devices, groups, columns)
    modulation = pick(modulation_all, 1, group).reshape(-1)
    shift_one, scale_one, gate_one, shift_two, scale_two, gate_two = [
        modulation[part * D : (part + 1) * D] for part in range(6)
    ]

    project_wide = jnp.concatenate(
        [
            pad_heads(project_mine[:, : 3 * HEADS * HD].reshape(D, 3 * HEADS, HD), 2).reshape(
                D, 3 * WIDE
            ),
            jnp.pad(project_mine[:, 3 * HEADS * HD :], ((0, 0), (0, LANES - HEADS))),
        ],
        axis=1,
    )
    expand_cut = (
        expander.reshape(depth, groups, TEAM, inner)
        .transpose(2, 0, 1, 3)
        .reshape(TEAM, depth, groups * inner)
    )
    expand_part = lax.all_to_all(expand_cut, "pos", split_axis=0, concat_axis=0, tiled=True)
    expand_mine = group_gather_in(expand_part).reshape(D, groups * inner)
    reduce_mine = group_gather_in(reducer)
    if whole_heads:
        combine_mine = group_gather_in(combiner).reshape(HEADS, HD, D)
    else:
        combine_all = lax.all_gather(combiner, rows_axes, axis=0, tiled=True)
        combine_mine = pick(combine_all.reshape(HEADS, TEAM, HD, D), 1, place)
    combine_wide = pad_heads(combine_mine, 1).reshape(WIDE, D)
    thresholds_mine = pick(thresholds.reshape(groups, TEAM, inner), 1, place).reshape(-1)
    retention_mine = pick(retention.reshape(HEADS, TEAM), 1, place)
    kernel = pad_heads(pick(smoother.reshape(9, HEADS, TEAM, HD), 2, place), 2).reshape(9, WIDE)
    offset = pad_heads(pick(pedestal.reshape(HEADS, TEAM, HD), 1, place), 1).reshape(WIDE)

    hidden = modulate(inputs, shift_one, scale_one).astype(BF16)
    reduced_grad = (gate_two * upstream).astype(BF16)
    hidden_all, reduced_grad_all = team_gather(hidden, reduced_grad)
    projected = dot(hidden_all, project_wide)
    forget_logit = projected[:, 3 * WIDE : 3 * WIDE + HEADS] + retention_mine
    decays = (jax.nn.log_sigmoid(forget_logit) / 16.0).astype(BF16)
    index = jnp.arange(PATCHES, dtype=jnp.int32)
    length = pick(lengths, 0, group)
    validity = (index < length)[:, None]
    is_query = jnp.arange(3 * WIDE) < WIDE
    keep = validity | is_query[None, :]
    qkv = jnp.where(keep, projected[:, : 3 * WIDE], 0.0).astype(BF16)
    order = column_place(index)
    causal = (order[None, :] <= order[:, None]).astype(BF16)
    summed = dot(causal, decays)
    gcol = summed.T[:, :, None]
    grow = summed.T[:, None, :]
    attended = attend(qkv, gcol, grow)

    attended_grid = attended.astype(F32).reshape(GRID, GRID, WIDE)
    attended_padded = pad_cells(attended_grid)
    smoothed = jnp.zeros_like(attended_grid) + offset
    for tap in range(9):
        down, right = tap // 3, tap % 3
        smoothed = (
            smoothed + kernel[tap] * attended_padded[down : down + GRID, right : right + GRID]
        )
    smoothed = smoothed.astype(BF16).reshape(PATCHES, WIDE)
    branch = team_scatter(dot(smoothed, combine_wide)) + displacement
    middle = inputs + gate_one * branch
    hidden_two = modulate(middle, shift_two, scale_two).astype(BF16)
    hidden_two_all = team_gather(hidden_two)
    expanded = dot(hidden_two_all, expand_mine) + thresholds_mine
    activated = jax.nn.gelu(expanded, approximate=True).astype(BF16)

    def swap_add(share):
        low = share.astype(BF16)
        other = lax.ppermute(low, "items", [(0, 1), (1, 0)])
        return low.astype(F32) + other.astype(F32)

    def to_owners(source):
        pieces = source.reshape(devices, depth, source.shape[1])
        arrived = lax.all_to_all(pieces, rows_axes, split_axis=0, concat_axis=0, tiled=True)
        arrived = arrived.reshape(groups, TEAM, depth, source.shape[1])
        return jnp.sum(arrived.astype(F32), axis=0).astype(BF16)

    def group_scatter_in(source):
        low = source.astype(BF16)
        if groups != 2:
            arrived = lax.all_to_all(low, "grp", split_axis=0, concat_axis=0, tiled=True)
            return jnp.sum(arrived.astype(F32), axis=0)
        arrived = lax.ppermute(pick(low, 0, 1 - group), "grp", [(0, 1), (1, 0)])
        return pick(low, 0, group).astype(F32) + arrived.astype(F32)

    leveling_grad = jnp.sum(reduced_grad.astype(F32), axis=0)
    reducer_grad = outer_sum(activated, reduced_grad_all)
    reducer_out = swap_add(group_scatter_in(reducer_grad.reshape(groups, inner, D)))
    activated_grad = back_dot(reduced_grad_all, reduce_mine)
    pull = jax.vjp(lambda v: jax.nn.gelu(v, approximate=True), expanded)[1]
    expanded_grad = pull(activated_grad)[0].astype(BF16)
    thresholds_grad = jnp.sum(expanded_grad.astype(F32), axis=0)
    expander_grad = outer_sum(hidden_two_all, expanded_grad)
    expander_out = swap_add(
        to_owners(expander_grad.astype(BF16))
        .reshape(TEAM, depth, groups, inner)
        .transpose(1, 2, 0, 3)
        .reshape(depth, FF),
    )
    hidden_two_grad, reduced = team_scatter(
        back_dot(expanded_grad, expand_mine), dot(activated, reduce_mine)
    )
    reduced = reduced + leveling
    block_output = (middle + gate_two * reduced).astype(BF16).reshape(ROWS_DEV, GRID, D)
    gate_two_grad = jnp.sum(upstream * reduced, axis=0)
    second_pull = jax.vjp(modulate, middle, shift_two, scale_two)[1]
    middle_part, shift_two_grad, scale_two_grad = second_pull(hidden_two_grad)
    middle_grad = upstream + middle_part
    gate_one_grad = jnp.sum(middle_grad * branch, axis=0)
    branch_grad = (gate_one * middle_grad).astype(BF16)
    displacement_grad = jnp.sum(branch_grad.astype(F32), axis=0)
    branch_grad_all = team_gather(branch_grad)
    combiner_grad = outer_sum(smoothed, branch_grad_all)
    combiner_low = combiner_grad.reshape(HEADS, LANES, D)[:, :HD]
    if whole_heads:
        combiner_share = group_scatter_in(combiner_low)
    else:
        placed = jnp.where(
            (jnp.arange(TEAM) == place)[None, :, None, None], combiner_low[:, None], 0.0
        )
        combiner_share = lax.psum_scatter(
            placed.reshape(D, D), rows_axes, scatter_dimension=0, tiled=True
        )
    combiner_out = swap_add(combiner_share)
    smoothed_grad = back_dot(branch_grad_all, combine_wide).astype(BF16).astype(F32)
    pedestal_grad = jnp.sum(smoothed_grad, axis=0)
    grad_grid = smoothed_grad.reshape(GRID, GRID, WIDE)
    grad_padded = pad_cells(grad_grid)
    tap_grads = []
    attended_grad = jnp.zeros_like(grad_grid)
    for tap in range(9):
        down, right = tap // 3, tap % 3
        tap_grads.append(
            jnp.sum(
                grad_grid * attended_padded[down : down + GRID, right : right + GRID], axis=(0, 1)
            )
        )
        attended_grad = (
            attended_grad
            + kernel[tap] * grad_padded[2 - down : 2 - down + GRID, 2 - right : 2 - right + GRID]
        )
    tap_stack = jnp.stack(tap_grads)
    attended_grad = attended_grad.astype(BF16).reshape(PATCHES, WIDE)
    dq, dk, dv, row_sum, col_sum = attend_back(qkv, gcol, grow, attended_grad)
    moment = row_sum[:, :, 0] - col_sum[:, 0, :]
    decay_grad = lax.dot_general(
        causal.astype(F32),
        moment,
        (((0,), (1,)), ((), ())),
        precision=HIGH,
        preferred_element_type=F32,
    )
    forget_grad = (decay_grad * jax.nn.sigmoid(-forget_logit) / 16.0).astype(BF16)
    retention_grad = jnp.sum(forget_grad.astype(F32), axis=0)
    project_grad = jnp.concatenate(
        [
            dq.astype(BF16),
            jnp.where(validity, dk, 0.0).astype(BF16),
            jnp.where(validity, dv, 0.0).astype(BF16),
            jnp.pad(forget_grad, ((0, 0), (0, LANES - HEADS))),
        ],
        axis=1,
    )
    projector_grad = outer_sum(hidden_all, project_grad)
    hidden_grad = team_scatter(back_dot(project_grad, project_wide))
    first_pull = jax.vjp(modulate, inputs, shift_one, scale_one)[1]
    inputs_part, shift_one_grad, scale_one_grad = first_pull(hidden_grad)
    patches_grad = (middle_grad + inputs_part).astype(BF16).reshape(ROWS_DEV, GRID, D)

    projector_low = projector_grad.astype(BF16)
    project_share = to_owners(
        jnp.concatenate(
            [
                projector_low[:, : 3 * WIDE].reshape(D, 3 * HEADS, LANES)[:, :, :HD].reshape(
                    D, 3 * HEADS * HD
                ),
                projector_low[:, 3 * WIDE : 3 * WIDE + HEADS],
            ],
            axis=1,
        ),
    )
    projector_out = swap_add(
        project_share[:, :, : 3 * HEADS * HD]
        .reshape(TEAM, depth, 3, HEADS, HD)
        .transpose(1, 2, 3, 0, 4)
        .reshape(depth, 3 * D),
    )
    forgetter_out = swap_add(
        project_share[:, :, 3 * HEADS * HD :].transpose(1, 2, 0).reshape(depth, H),
    )

    modulation_grad = jnp.concatenate(
        [
            shift_one_grad,
            scale_one_grad,
            gate_one_grad,
            shift_two_grad,
            scale_two_grad,
            gate_two_grad,
        ]
    ).reshape(devices, columns)
    rows_every = small_scatter(modulation_grad, (halves, groups), 8)
    modulator_out = lax.dot_general(
        squashed_every.astype(F32), rows_every, (((0,), (0,)), ((), ())), precision=HIGH
    )
    baseline_out = jnp.sum(rows_every, axis=0)
    modulation_rows = pick(rows_every.reshape(halves, groups, columns), 0, half)
    squashed_grad = jnp.dot(modulation_rows, modulator.astype(F32).T, precision=HIGH)

    def spot(value, shape, axis, at):
        where = (jnp.arange(shape[axis]) == at).reshape(
            [-1 if spot_axis == axis else 1 for spot_axis in range(len(shape))]
        )
        return jnp.where(where, jnp.expand_dims(value, axis), 0.0).reshape(-1)

    parts = [
        spot(squashed_grad, (halves, groups, D), 0, half),
        spot(retention_grad, (HEADS, TEAM), 1, place),
        spot(tap_stack.reshape(9, HEADS, LANES)[:, :, :HD], (9, HEADS, TEAM, HD), 2, place),
        spot(pedestal_grad.reshape(HEADS, LANES)[:, :HD], (HEADS, TEAM, HD), 1, place),
        displacement_grad,
        spot(thresholds_grad.reshape(groups, inner), (groups, TEAM, inner), 1, place),
        leveling_grad,
    ]
    total = small_sum(jnp.concatenate(parts), (halves, groups), 9)
    split = []
    start = 0
    for part in parts:
        split.append(total[start : start + part.shape[0]])
        start += part.shape[0]
    squashed_sum = pick(split[0].reshape(halves, groups, D), 0, half)
    silu_pull = jax.vjp(jax.nn.silu, condition_float)[1]
    condition_grad = silu_pull(squashed_sum)[0]
    return (
        block_output,
        patches_grad,
        condition_grad,
        modulator_out,
        baseline_out,
        projector_out,
        forgetter_out,
        split[1],
        split[2].reshape(9, D),
        split[3],
        combiner_out,
        split[4],
        expander_out,
        split[5],
        reducer_out,
        split[6],
    )


def solution(mesh):
    rows = mesh.shape["rows"]
    groups = rows // TEAM
    fine = Mesh(
        mesh.devices.reshape(mesh.shape["items"], groups, TEAM), ("items", "grp", "pos")
    )
    line = ("grp", "pos")
    tokens = P(("items", "grp", "pos"), None, None)
    in_specs = (
        tokens,
        P("items", None),
        P("items"),
        P(None, line),
        P(line),
        P(line, None),
        P(line, None),
        P(),
        P(),
        P(),
        P(line, None),
        P(),
        P(line, None),
        P(),
        P(line, None),
        P(),
        tokens,
    )
    out_specs = (
        tokens,
        tokens,
        P("items", None),
        P(None, line),
        P(line),
        P(line, None),
        P(line, None),
        P(),
        P(),
        P(),
        P(line, None),
        P(),
        P(line, None),
        P(),
        P(line, None),
        P(),
    )
    return jax.shard_map(
        functools.partial(on_device, groups),
        mesh=fine,
        in_specs=in_specs,
        out_specs=out_specs,
        check_vma=False,
    )
```
